1024 devices in a mesh: section: 16 (over y, z_hi), ctx: 64 (over z_lo, x, core).
Axes of the slice: x: 4, y: 4, z: 32 (z_hi: 4, z_lo: 8; z = z_hi * 8 + z_lo), core: 2. Of those that a mesh axis runs over, the one named last changes fastest.
Arguments:
- queries: bfloat16 [16, 8, 8192, 512], P('section', None, 'ctx'), may hold values from -5 to 5
- keys: bfloat16 [16, 8, 8192, 128], P('section', None, 'ctx'), may hold values from -5 to 5
- values: bfloat16 [16, 8, 8192, 128], P('section', None, 'ctx'), may hold values from -6 to 6
- out_grad: bfloat16 [16, 8192, 512], P('section', 'ctx'), may hold values from -6 to 6
- stretch_ids: int32 [128], P('ctx'), may hold values from 0 to 127, as said below
- stash_slot: int32 [16], P('section'), may hold values from 0 to 7
Outputs:
- passed_grads: bfloat16 [16, 8192, 768], P('section', 'ctx')
The draws below stay inside these ranges and needn't reach their ends.
Inputs may be any that keep to these rules, and one draw needn't show every extreme that they name: `stretch_ids`: for each sequence, the entries of its 64 row blocks (two a block, blocks in order) are a permutation of 0 to 127 in which a block's two entries are some c and 127 - c, in either order.
All inputs are finite; a program needn't handle non-finite values.
Results may differ from the reference program's by a relative error of at most 0.035.
Values may be sent and summed in bfloat16 or wider, within the bound.
A program may use at most 64 MiB of HBM per device.

```python
import math
import jax
import jax.numpy as jnp
from jax import lax

GROUP = 4
HEAD = 128
TOK_DEV = 128
SEQS = 1
MICRO = 8
HALF = 64
SPAN = 64
STRETCHES = 128
TOKENS = 8192
LENGTH = 8192
SECTIONS = 16
QW = 512


def draw_queries(key, part):
    shape = (SECTIONS, MICRO, TOKENS, GROUP * HEAD)
    return jax.random.truncated_normal(jax.random.fold_in(key, 7), -5.0, 5.0, shape, jnp.float32).astype(jnp.bfloat16)


def draw_keys(key, part):
    shape = (SECTIONS, MICRO, TOKENS, HEAD)
    return jax.random.truncated_normal(jax.random.fold_in(key, 17), -5.0, 5.0, shape, jnp.float32).astype(jnp.bfloat16)


def sequence_stretches(seq_key):
    order = jax.random.permutation(jax.random.fold_in(seq_key, 1), SPAN).astype(jnp.int32)
    flips = jax.random.randint(jax.random.fold_in(seq_key, 2), (SPAN,), 0, 2).astype(jnp.int32)
    mirror = (2 * SPAN - 1 - order).astype(jnp.int32)
    first = jnp.where(flips == 1, mirror, order)
    second = jnp.where(flips == 1, order, mirror)
    return jnp.stack([first, second], axis=1).astype(jnp.int32)


def draw_stretch_ids(key, part):
    seq_keys = jax.random.split(jax.random.fold_in(key, 11), SEQS)
    per_seq = jax.vmap(sequence_stretches)(seq_keys)
    return jnp.swapaxes(per_seq, 0, 1).reshape(STRETCHES).astype(jnp.int32)


def place_ends(entries, key, smallest, largest):
    spot = [jax.random.randint(jax.random.fold_in(key, axis), (), 0, length) for axis, length in enumerate(entries.shape)]
    main_axis = entries.shape.index(max(entries.shape))
    neighbour = spot[:main_axis] + [(spot[main_axis] + 1) % entries.shape[main_axis]] + spot[main_axis + 1:]
    return entries.at[tuple(spot)].set(smallest).at[tuple(neighbour)].set(largest)


def steps_of(own_key, shape, cuts, smallest, high):
    loudness, own = 1.0, jax.random.fold_in(own_key, 6)
    for axis_at, shards_of in cuts:
        draws = jnp.exp(jax.random.uniform(jax.random.fold_in(own, axis_at), (shards_of,), jnp.float32, smallest / len(cuts), high / len(cuts)))
        loudness = loudness * jnp.repeat(draws, shape[axis_at] // shards_of).reshape([-1 if axis == axis_at else 1 for axis in range(len(shape))])
    return loudness


def bell_draw(rng, extent, width, most, shards=(), kind=jnp.bfloat16):
    level = steps_of(rng, extent, shards, -0.22, 0.18) if shards else 1.0
    result = jax.random.normal(rng, extent, jnp.float32) * width * level
    return jnp.minimum(jnp.maximum(result, -most), most).astype(kind)


def setup_inputs(seed: int = 0) -> dict:
    splits = jax.random.split(jax.random.key(seed), 7)
    queries = draw_queries(jax.random.fold_in(splits[6], 71), 0)
    keys = draw_keys(jax.random.fold_in(splits[6], 71), 0)
    values = bell_draw(splits[2], (SECTIONS, MICRO, TOKENS, HEAD), 1.0, 6.0, ((0, 16), (2, 64)))
    out_grad = bell_draw(splits[3], (SECTIONS, TOKENS, QW), 1.0, 6.0, ((0, 16), (1, 64)))
    stretch_ids = draw_stretch_ids(jax.random.fold_in(splits[6], 71), 0)
    stash_slot = place_ends(jax.random.randint(splits[5], (SECTIONS,), 0, MICRO), jax.random.fold_in(splits[5], 1), 0, MICRO - 1).astype(jnp.int32)
    return dict(queries=queries, keys=keys, values=values, out_grad=out_grad, stretch_ids=stretch_ids, stash_slot=stash_slot)


def section_message(query_all, key_all, value_all, grad_all, token_place):
    softmax_scale = 1.0 / math.sqrt(HEAD)
    block_width = math.gcd(LENGTH, 256)
    blocks = LENGTH // block_width
    key_wide = key_all.astype(jnp.float32)
    value_wide = value_all.astype(jnp.float32)

    def one_block(sums_now, block_index):
        start = block_index * block_width
        query_rows = lax.dynamic_slice_in_dim(query_all, start, block_width, 0).astype(jnp.float32).reshape(block_width, GROUP, HEAD)
        grad_rows = lax.dynamic_slice_in_dim(grad_all, start, block_width, 0).astype(jnp.float32).reshape(block_width, GROUP, HEAD)
        query_place = lax.dynamic_slice_in_dim(token_place, start, block_width, 0)
        visible = token_place[None, None, :] <= query_place[:, None, None]
        scores = jnp.einsum('thd,cd->thc', query_rows, key_wide) * softmax_scale
        scores = jnp.where(visible, scores, -jnp.inf)
        row_top = lax.optimization_barrier(jnp.max(scores, axis=2, keepdims=True))
        log_total = row_top + jnp.log(lax.optimization_barrier(jnp.sum(jnp.exp(scores - row_top), axis=2, keepdims=True)))
        weights = jnp.exp(scores - log_total)
        probs_half = lax.optimization_barrier(weights.astype(jnp.bfloat16)).astype(jnp.float32)
        attention = jnp.einsum('thc,cd->thd', probs_half, value_wide)
        row_delta = lax.optimization_barrier(jnp.sum(grad_rows * attention, axis=2, keepdims=True))
        prob_grad = jnp.einsum('thd,cd->thc', grad_rows, value_wide)
        score_grad = lax.optimization_barrier((softmax_scale * weights * (prob_grad - row_delta)).astype(jnp.bfloat16)).astype(jnp.float32)
        query_grad = jnp.einsum('thc,cd->thd', score_grad, key_wide)
        key_grad = sums_now[0] + jnp.einsum('thc,thd->cd', score_grad, query_rows)
        value_grad = sums_now[1] + jnp.einsum('thc,thd->cd', probs_half, grad_rows)
        return ((key_grad, value_grad), query_grad.reshape(block_width, GROUP * HEAD))
    zero_rows = jnp.zeros((LENGTH, HEAD), jnp.float32)
    final_sums, query_grad = lax.scan(one_block, (zero_rows, zero_rows), jnp.arange(blocks, dtype=jnp.int32))
    query_grad = query_grad.reshape(LENGTH, GROUP * HEAD)
    return jnp.concatenate([query_grad, final_sums[0], final_sums[1]], axis=1).astype(jnp.bfloat16)

def regroup(array):
    tail = array.shape[1:]
    return jnp.swapaxes(array.reshape((SPAN, SEQS, TOK_DEV) + tail), 0, 1).reshape((SEQS, LENGTH) + tail)

def ungroup(array):
    tail = array.shape[2:]
    return jnp.swapaxes(array.reshape((SEQS, SPAN, TOK_DEV) + tail), 0, 1).reshape((TOKENS,) + tail)

def reference(queries, keys, values, out_grad, stretch_ids, stash_slot):
    row_ids = jnp.arange(TOKENS, dtype=jnp.int32)
    token_place = regroup(stretch_ids[row_ids // HALF] * HALF + row_ids % HALF)

    def per_section(section_index):
        stash_index = stash_slot[section_index]
        query_seq = regroup(queries[section_index, stash_index])
        key_seq = regroup(keys[section_index, stash_index])
        value_seq = regroup(values[section_index, stash_index])
        grad_seq = regroup(out_grad[section_index])

        def per_sequence(seq_index):
            return section_message(query_seq[seq_index], key_seq[seq_index], value_seq[seq_index], grad_seq[seq_index], token_place[seq_index])
        return ungroup(lax.map(per_sequence, jnp.arange(SEQS, dtype=jnp.int32)))
    messages = lax.map(per_section, jnp.arange(SECTIONS, dtype=jnp.int32))
    return jnp.roll(messages, -1, axis=0)
```

```python
import functools
import math

import jax
import jax.numpy as jnp
from jax import lax
from jax.experimental import pallas as pl
from jax.experimental.pallas import tpu as pltpu
from jax.sharding import Mesh
from jax.sharding import PartitionSpec as P

Z, X, CORE, SECTION = "ctx_0", "ctx_1", "ctx_2", "section"
CTX = (Z, X, CORE)
MESH = pl.DeviceIdType.MESH
VMEM = pl.BlockSpec(memory_space=pltpu.VMEM)
SMEM = pl.BlockSpec(memory_space=pltpu.SMEM)
ANY = pl.BlockSpec(memory_space=pl.ANY)
DMA = pltpu.SemaphoreType.DMA
VMEM_LIMIT = 60 * 1024 * 1024

ID_ROWS = 16
masked_score = -1e30


def neighbours(nz, nx):
    z, x, core = lax.axis_index(Z), lax.axis_index(X), lax.axis_index(CORE)
    right = lax.rem(x + 1, nx)
    left = lax.rem(x + nx - 1, nx)
    far = lax.rem(x + nx // 2, nx)
    return z, x, core, right, left, far


def greet(nz, z, core, right, left, more=0):
    barrier = pltpu.get_barrier_semaphore()

    def signal(**where):
        pl.semaphore_signal(barrier, inc=1, device_id=dict(where), device_id_type=MESH)

    signal(**{X: right})
    signal(**{X: left})
    signal(**{CORE: 1 - core})

    @pl.when(z > 0)
    def _():
        signal(**{Z: z - 1})

    @pl.when(z < nz - 1)
    def _():
        signal(**{Z: z + 1})

    inside = (z > 0).astype(jnp.int32) + (z < nz - 1).astype(jnp.int32)
    pl.semaphore_wait(barrier, 3 + more + inside)


def remote(src, dst, send, recv, where):
    return pltpu.make_async_remote_copy(
        src_ref=src, dst_ref=dst, send_sem=send, recv_sem=recv, device_id=where, device_id_type=MESH
    )


def gather_kernel(nz, nx, blk, out, zs, zr, xs, xr, hs, hr, ps, pr, own_sem):
    z, x, core, right, left, far = neighbours(nz, nx)
    rows = blk.shape[0]
    cut = rows // 2 // 16 * 16
    halves = (pl.ds(0, cut), pl.ds(cut, rows - cut))

    def slot(zz, xx, cc):
        return (zz * nx + xx) * 2 + cc

    own = pltpu.make_async_copy(blk, out.at[slot(z, x, core)], own_sem)
    own.start()
    greet(nz, z, core, right, left)

    def along_z(src, zz, up):
        to = z + 1 if up else z - 1
        return remote(src, out.at[slot(zz, x, core)], zs.at[0 if up else 1, zz], zr.at[zz], {Z: to})

    def along_x(src, zz, xx, way):
        to = right if way == 0 else left
        return remote(src, out.at[slot(zz, xx, core)], xs.at[way, zz], xr.at[way, zz], {X: to})

    def half_on(zz, xx, way):
        to = right if way == 0 else left
        piece = out.at[slot(zz, xx, core), halves[way]]
        return remote(piece, piece, hs.at[way, zz], hr.at[way, zz], {X: to})

    def across(src, zz, xx):
        at = zz * nx + xx
        return remote(src, out.at[slot(zz, xx, core)], ps.at[at], pr.at[at], {CORE: 1 - core})

    def here(zz, xx):
        return out.at[slot(zz, xx, core)]

    def spread(src, zz):
        along_x(src, zz, x, 0).start()
        along_x(src, zz, x, 1).start()
        across(src, zz, x).start()

    @pl.when(z < nz - 1)
    def _():
        along_z(blk, z, True).start()

    @pl.when(z > 0)
    def _():
        along_z(blk, z, False).start()

    spread(blk, z)

    def z_stage(s):
        @pl.when(z - s >= 0)
        def _():
            zz = z - s
            along_z(here(zz, x), zz, True).wait_recv()

            @pl.when(z < nz - 1)
            def _():
                along_z(here(zz, x), zz, True).start()

            spread(here(zz, x), zz)

        @pl.when(z + s <= nz - 1)
        def _():
            zz = z + s
            along_z(here(zz, x), zz, False).wait_recv()

            @pl.when(z > 0)
            def _():
                along_z(here(zz, x), zz, False).start()

            spread(here(zz, x), zz)

    def x_one(zz):
        along_x(here(zz, left), zz, left, 0).wait_recv()
        half_on(zz, left, 0).start()
        across(here(zz, left), zz, left).start()
        along_x(here(zz, right), zz, right, 1).wait_recv()
        half_on(zz, right, 1).start()
        across(here(zz, right), zz, right).start()

    def h_one(zz):
        half_on(zz, far, 0).wait_recv()
        half_on(zz, far, 1).wait_recv()
        across(here(zz, far), zz, far).start()

    def both_ways(one, t):
        @pl.when(z - t >= 0)
        def _():
            one(z - t)

        @pl.when((t > 0) & (z + t <= nz - 1))
        def _():
            one(z + t)

    def step(s, _):
        @pl.when(s < nz)
        def _():
            z_stage(s)

        @pl.when(s <= nz)
        def _():
            both_ways(x_one, s - 1)

        @pl.when(s >= 2)
        def _():
            both_ways(h_one, s - 2)

        return 0

    lax.fori_loop(1, nz + 2, step, 0)

    def drain(zz, _):
        @pl.when((zz <= z) & (z < nz - 1))
        def _():
            along_z(here(zz, x), zz, True).wait_send()

        @pl.when((zz >= z) & (z > 0))
        def _():
            along_z(here(zz, x), zz, False).wait_send()

        for way in (0, 1):
            along_x(here(zz, x), zz, x, way).wait_send()
            half_on(zz, left if way == 0 else right, way).wait_send()
        for xx in range(nx):
            across(here(zz, xx), zz, xx).wait_send()
            at = zz * nx + xx
            other = out.at[slot(zz, xx, 1 - core)]
            remote(other, other, ps.at[at], pr.at[at], {CORE: 1 - core}).wait_recv()
        return 0

    lax.fori_loop(0, nz, drain, 0)
    own.wait()


def gathered(blk, nz, nx):
    shape = (nz * nx * 2, *blk.shape)
    return pl.pallas_call(
        functools.partial(gather_kernel, nz, nx),
        out_shape=jax.ShapeDtypeStruct(shape, blk.dtype),
        in_specs=[VMEM],
        out_specs=VMEM,
        scratch_shapes=[
            DMA((2, nz)),
            DMA((nz,)),
            DMA((2, nz)),
            DMA((2, nz)),
            DMA((2, nz)),
            DMA((2, nz)),
            DMA((nz * nx,)),
            DMA((nz * nx,)),
            DMA,
        ],
        compiler_params=pltpu.CompilerParams(
            collective_id=0, has_side_effects=True, vmem_limit_bytes=VMEM_LIMIT
        ),
        name="gather",
    )(blk)


def attend_kernel(
    group,
    head,
    half,
    scale,
    stash,
    ids,
    own_ids,
    queries,
    grads,
    blocks,
    dq,
    dkv,
    q_full,
    qs,
    gs,
    tops,
    totals,
    deltas,
    dq_sum,
    scores,
    dprobs,
    where_is,
    sem,
):
    total = ids.shape[0]
    per = 256 // half
    tiles = total // per
    rows = group * half
    fetch = pltpu.make_async_copy(queries.at[0, stash[0]], q_full, sem)
    fetch.start()

    def place(i, _):
        where_is[ids[i]] = i
        return 0

    lax.fori_loop(0, total, place, 0)
    low_first = (own_ids[0] < own_ids[1]).astype(jnp.int32)
    low = jnp.minimum(own_ids[0], own_ids[1])
    high = total - 1 - low
    halves = (low_first * half, (1 - low_first) * half)
    fetch.wait()
    for p in (0, 1):
        base = pl.multiple_of(halves[p], half)
        for h in range(group):
            cols = slice(h * head, (h + 1) * head)
            qs[p, h * half : (h + 1) * half, :] = q_full[pl.ds(base, half), cols]
            gs[p, h * half : (h + 1) * half, :] = grads[0, pl.ds(base, half), cols]
    tops[...] = jnp.full_like(tops, masked_score)
    totals[...] = jnp.zeros_like(totals)
    deltas[...] = jnp.zeros_like(deltas)
    dq_sum[...] = jnp.zeros_like(dq_sum)

    high_tiles = high // per + 1
    exp_scale = scale * math.log2(math.e)
    gap = lax.broadcasted_iota(jnp.int32, (256, rows), 0) - (
        lax.broadcasted_iota(jnp.int32, (256, rows), 1) % half
    )

    def unit(u):
        p = (u >= high_tiles).astype(jnp.int32)
        return p, u - p * high_tiles

    def tile_of(tile, first):
        pieces = []
        for i in range(per):
            at = where_is[tile * per + i]
            start = pl.multiple_of(first + (at % 2) * half, half)
            pieces.append(blocks[at // 2, pl.ds(start, half), :])
        return jnp.concatenate(pieces, axis=0)

    def cross(a, b, dims):
        return lax.dot_general(a, b, (dims, ((), ())), preferred_element_type=jnp.float32)

    def forward(u):
        p, tile = unit(u)
        mine = jnp.where(p == 0, high, low)
        t = cross(tile_of(tile, 0), qs[p], ((1,), (1,))) * exp_scale
        t = jnp.where(gap <= mine * half - tile * 256, t, masked_score)
        dprob = cross(tile_of(tile, 2 * half), gs[p], ((1,), (1,)))
        scores[u] = t
        dprobs[u] = dprob
        old = tops[p]
        new = jnp.maximum(old, jnp.max(t, axis=0, keepdims=True))
        fading = jnp.exp2(old - new)
        e = jnp.exp2(t - new)
        tops[p] = new
        totals[p] = totals[p] * fading + jnp.sum(e, axis=0, keepdims=True)
        deltas[p] = deltas[p] * fading + jnp.sum(e * dprob, axis=0, keepdims=True)

    units = tiles + 1
    together = 3 if units % 3 == 0 else 1

    def forward_step(i, _):
        for k in range(together):
            forward(i * together + k)
        return 0

    lax.fori_loop(0, units // together, forward_step, 0)
    deltas[...] = deltas[...] / totals[...]
    tops[...] = tops[...] + jnp.log2(totals[...])

    def backward(u):
        p, tile = unit(u)
        weights = jnp.exp2(scores[u] - tops[p])
        probs = weights.astype(jnp.bfloat16)
        dscore = (weights * (dprobs[u] - deltas[p]) * scale).astype(jnp.bfloat16)
        dk = cross(dscore, qs[p], ((1,), (0,)))
        dv = cross(probs, gs[p], ((1,), (0,)))
        dq_sum[p] += cross(tile_of(tile, 0), dscore, ((0,), (0,)))
        for i in range(per):
            at = where_is[tile * per + i]
            here = slice(i * half, (i + 1) * half)
            for part, first in ((dk, 0), (dv, 2 * half)):
                spot = (at // 2, pl.ds(pl.multiple_of(first + (at % 2) * half, half), half))
                before = jnp.where(p == 1, dkv[spot].astype(jnp.float32), 0.0)
                dkv[spot] = (before + part[here]).astype(jnp.bfloat16)

    def backward_step(i, _):
        for k in range(together):
            backward(i * together + k)
        return 0

    lax.fori_loop(0, units // together, backward_step, 0)

    def clear(s, _):
        at = where_is[s]
        for first in (0, 2 * half):
            spot = (at // 2, pl.ds(pl.multiple_of(first + (at % 2) * half, half), half))
            dkv[spot] = jnp.zeros((half, head), jnp.bfloat16)
        return 0

    lax.fori_loop(high_tiles * per, total, clear, 0)
    for p in (0, 1):
        base = pl.multiple_of(halves[p], half)
        turned = dq_sum[p].T.astype(jnp.bfloat16)
        for h in range(group):
            dq[pl.ds(base, half), h * head : (h + 1) * head] = turned[h * half : (h + 1) * half]


def attended(stash, ids, own_ids, queries, grads, blocks, head):
    tokens, width = queries.shape[2:]
    group, half = width // head, tokens // 2
    rows = group * half
    units = ids.shape[0] * half // 256 + 1
    return pl.pallas_call(
        functools.partial(attend_kernel, group, head, half, 1.0 / math.sqrt(head)),
        out_shape=(
            jax.ShapeDtypeStruct((tokens, width), jnp.bfloat16),
            jax.ShapeDtypeStruct((blocks.shape[0], 2 * tokens, head), jnp.bfloat16),
        ),
        in_specs=[SMEM, SMEM, SMEM, ANY, VMEM, VMEM],
        out_specs=(VMEM, VMEM),
        scratch_shapes=[
            pltpu.VMEM((tokens, width), jnp.bfloat16),
            pltpu.VMEM((2, rows, head), jnp.bfloat16),
            pltpu.VMEM((2, rows, head), jnp.bfloat16),
            pltpu.VMEM((2, 1, rows), jnp.float32),
            pltpu.VMEM((2, 1, rows), jnp.float32),
            pltpu.VMEM((2, 1, rows), jnp.float32),
            pltpu.VMEM((2, head, rows), jnp.float32),
            pltpu.VMEM((units, 256, rows), jnp.float32),
            pltpu.VMEM((units, 256, rows), jnp.float32),
            pltpu.SMEM((ids.shape[0],), jnp.int32),
            DMA,
        ],
        compiler_params=pltpu.CompilerParams(vmem_limit_bytes=VMEM_LIMIT),
        name="attend",
    )(stash, ids, own_ids, queries, grads, blocks)


def scatter_kernel(
    nz, nx, ns, dq, dkv, out, rx, held, hbuf, xbuf, zbuf, last, ps, pr, hs, hr, xs, xr, zs, zr, ms, mr
):
    z, x, core, right, left, far = neighbours(nz, nx)
    section = lax.axis_index(SECTION)
    ahead = lax.rem(section + ns - 1, ns)
    behind = lax.rem(section + 1, ns)
    tokens, width = dq.shape
    head = dkv.shape[2]
    ways = (right, left)

    barrier = pltpu.get_barrier_semaphore()
    pl.semaphore_signal(barrier, inc=1, device_id={SECTION: behind}, device_id_type=MESH)
    greet(nz, z, core, right, left, more=1)

    def pair(zz, xx):
        at = zz * nx + xx
        src = dkv.at[at * 2 + 1 - core]
        return remote(src, rx.at[at], ps.at[at], pr.at[at], {CORE: 1 - core})

    def nth(k):
        return jnp.where(k % 2 == 0, k // 2, nz - 1 - k // 2)

    main = remote(dq, out.at[:, pl.ds(0, width)], ms.at[0], mr.at[0], {SECTION: ahead})

    def launch(k, _):
        for xx in range(nx):
            pair(nth(k), xx).start()
        return 0

    lax.fori_loop(0, nz, launch, 0)
    main.start()

    def mine(zz, xx):
        at = zz * nx + xx
        return dkv[at * 2 + core].astype(jnp.float32) + rx[at].astype(jnp.float32)

    def half_on(zz, way):
        piece = held.at[zz, 0, pl.ds(way * tokens, tokens)]
        return remote(piece, hbuf.at[way, zz], hs.at[way, zz], hr.at[way, zz], {X: ways[way]})

    def along_x(zz, way):
        return remote(
            held.at[zz, 1 + way], xbuf.at[way, zz], xs.at[way, zz], xr.at[way, zz], {X: ways[way]}
        )

    def first(zz):
        for xx in range(nx):
            pair(zz, xx).wait_recv()
        held[zz, 0] = mine(zz, far).astype(jnp.bfloat16)
        half_on(zz, 0).start()
        half_on(zz, 1).start()

    def second(zz):
        for way in (0, 1):
            half_on(zz, way).wait_recv()
            own = mine(zz, ways[way])
            more = hbuf[way, zz].astype(jnp.float32)
            keep = (1 - way) * tokens
            joined = own[way * tokens : (way + 1) * tokens] + more
            held[zz, 1 + way, way * tokens : (way + 1) * tokens] = joined.astype(jnp.bfloat16)
            held[zz, 1 + way, keep : keep + tokens] = own[keep : keep + tokens].astype(jnp.bfloat16)
            along_x(zz, way).start()

    def third(zz):
        along_x(zz, 0).wait_recv()
        along_x(zz, 1).wait_recv()
        done = mine(zz, x) + xbuf[0, zz].astype(jnp.float32) + xbuf[1, zz].astype(jnp.float32)
        held[zz, 3] = done.astype(jnp.bfloat16)

    def step(k, _):
        @pl.when(k < nz)
        def _():
            first(nth(k))

        @pl.when((k >= 1) & (k <= nz))
        def _():
            second(nth(k - 1))

        @pl.when(k >= 2)
        def _():
            third(nth(k - 2))

        return 0

    lax.fori_loop(0, nz + 2, step, 0)

    pieces = (pl.ds(0, tokens), pl.ds(tokens, tokens))

    def along_z(zz, down, piece):
        to = z - 1 if down else z + 1
        way = 0 if down else 1
        return remote(
            held.at[zz, 3, pieces[piece]],
            zbuf.at[way, zz, pieces[piece]],
            zs.at[way, zz, piece],
            zr.at[way, zz, piece],
            {Z: to},
        )

    def chain(zz, down, source):
        way = 0 if down else 1
        for piece in (0, 1):

            @pl.when(source)
            def _():
                along_z(zz, down, piece).wait_recv()
                joined = held[zz, 3, pieces[piece]].astype(jnp.float32) + zbuf[
                    way, zz, pieces[piece]
                ].astype(jnp.float32)
                held[zz, 3, pieces[piece]] = joined.astype(jnp.bfloat16)

            along_z(zz, down, piece).start()

    def chains(i, _):
        @pl.when(i < z)
        def _():
            chain(i, True, z < nz - 1)

        @pl.when(nz - 1 - i > z)
        def _():
            chain(nz - 1 - i, False, z > 0)

        return 0

    lax.fori_loop(0, nz - 1, chains, 0)

    for piece in (0, 1):
        last[pieces[piece]] = held[z, 3, pieces[piece]].astype(jnp.float32)

        @pl.when(z < nz - 1)
        def _():
            along_z(z, True, piece).wait_recv()
            last[pieces[piece]] += zbuf[0, z, pieces[piece]].astype(jnp.float32)

        @pl.when(z > 0)
        def _():
            along_z(z, False, piece).wait_recv()
            last[pieces[piece]] += zbuf[1, z, pieces[piece]].astype(jnp.float32)

        held[z, 3, pieces[piece]] = last[pieces[piece]].astype(jnp.bfloat16)

    def tail(piece):
        return remote(
            held.at[z, 3, pieces[piece]],
            out.at[:, pl.ds(width + piece * head, head)],
            ms.at[1 + piece],
            mr.at[1 + piece],
            {SECTION: ahead},
        )

    for piece in (0, 1):
        tail(piece).start()

    def drain(zz, _):
        for xx in range(nx):
            pair(zz, xx).wait_send()
        for way in (0, 1):
            half_on(zz, way).wait_send()
            along_x(zz, way).wait_send()
        for piece in (0, 1):

            @pl.when(zz < z)
            def _():
                along_z(zz, True, piece).wait_send()

            @pl.when(zz > z)
            def _():
                along_z(zz, False, piece).wait_send()

        return 0

    lax.fori_loop(0, nz, drain, 0)
    main.wait()
    for piece in (0, 1):
        tail(piece).wait()


def scattered(dq, dkv, nz, nx, ns):
    tokens, width = dq.shape
    rows, head = dkv.shape[1:]
    half = jnp.bfloat16
    return pl.pallas_call(
        functools.partial(scatter_kernel, nz, nx, ns),
        out_shape=jax.ShapeDtypeStruct((tokens, width + 2 * head), half),
        in_specs=[VMEM, VMEM],
        out_specs=VMEM,
        scratch_shapes=[
            pltpu.VMEM((nz * nx, rows, head), half),
            pltpu.VMEM((nz, 4, rows, head), half),
            pltpu.VMEM((2, nz, rows // 2, head), half),
            pltpu.VMEM((2, nz, rows, head), half),
            pltpu.VMEM((2, nz, rows, head), half),
            pltpu.VMEM((rows, head), jnp.float32),
            DMA((nz * nx,)),
            DMA((nz * nx,)),
            DMA((2, nz)),
            DMA((2, nz)),
            DMA((2, nz)),
            DMA((2, nz)),
            DMA((2, nz, 2)),
            DMA((2, nz, 2)),
            DMA((3,)),
            DMA((3,)),
        ],
        compiler_params=pltpu.CompilerParams(
            collective_id=1, has_side_effects=True, vmem_limit_bytes=VMEM_LIMIT
        ),
        name="scatter",
    )(dq, dkv)


def per_device(sizes, queries, keys, values, out_grad, stretch_ids, stash_slot):
    ns, nz, nx = sizes
    stash_index = stash_slot[0]
    key_rows = lax.dynamic_index_in_dim(keys[0], stash_index, 0, keepdims=False)
    value_rows = lax.dynamic_index_in_dim(values[0], stash_index, 0, keepdims=False)
    head = key_rows.shape[1]
    lane = lax.broadcasted_iota(jnp.int32, (ID_ROWS, head), 1)
    id_rows = jnp.where(lane < head // 2, stretch_ids[0], stretch_ids[1]).astype(jnp.bfloat16)
    blk = jnp.concatenate([key_rows, value_rows, id_rows], axis=0)
    blocks = gathered(blk, nz, nx)
    ids = blocks[:, 2 * key_rows.shape[0], :: head // 2].astype(jnp.int32).reshape(-1)
    dq, dkv = attended(stash_slot, ids, stretch_ids, queries, out_grad, blocks, head)
    return scattered(dq, dkv, nz, nx, ns)[None]


def solution(mesh):
    ns = mesh.shape["section"]
    nz, nx = 8, 4
    split = Mesh(mesh.devices.reshape(ns, nz, nx, 2), (SECTION, Z, X, CORE))
    return jax.shard_map(
        functools.partial(per_device, (ns, nz, nx)),
        mesh=split,
        in_specs=(
            P(SECTION, None, CTX, None),
            P(SECTION, None, CTX, None),
            P(SECTION, None, CTX, None),
            P(SECTION, CTX, None),
            P(CTX),
            P(SECTION),
        ),
        out_specs=P(SECTION, CTX, None),
        check_vma=False,
    )
```

```python
import functools
import math

import jax
import jax.numpy as jnp
from jax import lax
from jax.experimental import pallas as pl
from jax.experimental.pallas import tpu as pltpu
from jax.sharding import Mesh
from jax.sharding import PartitionSpec as P

Z, X, CORE, SECTION = "ctx_0", "ctx_1", "ctx_2", "section"
CTX = (Z, X, CORE)
MESH = pl.DeviceIdType.MESH
VMEM = pl.BlockSpec(memory_space=pltpu.VMEM)
SMEM = pl.BlockSpec(memory_space=pltpu.SMEM)
ANY = pl.BlockSpec(memory_space=pl.ANY)
DMA = pltpu.SemaphoreType.DMA
VMEM_LIMIT = 60 * 1024 * 1024

ID_ROWS = 16
masked_score = -1e30


def neighbours(nz, nx):
    z, x, core = lax.axis_index(Z), lax.axis_index(X), lax.axis_index(CORE)
    right = lax.rem(x + 1, nx)
    left = lax.rem(x + nx - 1, nx)
    far = lax.rem(x + nx // 2, nx)
    return z, x, core, right, left, far


def greet(nz, z, core, right, left, more=0):
    barrier = pltpu.get_barrier_semaphore()

    def signal(**where):
        pl.semaphore_signal(barrier, inc=1, device_id=dict(where), device_id_type=MESH)

    signal(**{X: right})
    signal(**{X: left})
    signal(**{CORE: 1 - core})

    @pl.when(z > 0)
    def _():
        signal(**{Z: z - 1})

    @pl.when(z < nz - 1)
    def _():
        signal(**{Z: z + 1})

    inside = (z > 0).astype(jnp.int32) + (z < nz - 1).astype(jnp.int32)
    pl.semaphore_wait(barrier, 3 + more + inside)


def remote(src, dst, send, recv, where):
    return pltpu.make_async_remote_copy(
        src_ref=src, dst_ref=dst, send_sem=send, recv_sem=recv, device_id=where, device_id_type=MESH
    )


def gather_kernel(nz, nx, blk, out, zs, zr, xs, xr, hs, hr, ps, pr, own_sem):
    z, x, core, right, left, far = neighbours(nz, nx)
    rows = blk.shape[0]
    cut = rows // 2 // 16 * 16
    halves = (pl.ds(0, cut), pl.ds(cut, rows - cut))

    def slot(zz, xx, cc):
        return (zz * nx + xx) * 2 + cc

    own = pltpu.make_async_copy(blk, out.at[slot(z, x, core)], own_sem)
    own.start()
    greet(nz, z, core, right, left)

    def along_z(src, zz, up):
        to = z + 1 if up else z - 1
        return remote(src, out.at[slot(zz, x, core)], zs.at[0 if up else 1, zz], zr.at[zz], {Z: to})

    def along_x(src, zz, xx, way):
        to = right if way == 0 else left
        return remote(src, out.at[slot(zz, xx, core)], xs.at[way, zz], xr.at[way, zz], {X: to})

    def half_on(zz, xx, way):
        to = right if way == 0 else left
        piece = out.at[slot(zz, xx, core), halves[way]]
        return remote(piece, piece, hs.at[way, zz], hr.at[way, zz], {X: to})

    def across(src, zz, xx):
        at = zz * nx + xx
        return remote(src, out.at[slot(zz, xx, core)], ps.at[at], pr.at[at], {CORE: 1 - core})

    def here(zz, xx):
        return out.at[slot(zz, xx, core)]

    def spread(src, zz):
        along_x(src, zz, x, 0).start()
        along_x(src, zz, x, 1).start()
        across(src, zz, x).start()

    @pl.when(z < nz - 1)
    def _():
        along_z(blk, z, True).start()

    @pl.when(z > 0)
    def _():
        along_z(blk, z, False).start()

    spread(blk, z)

    def z_stage(s):
        @pl.when(z - s >= 0)
        def _():
            zz = z - s
            along_z(here(zz, x), zz, True).wait_recv()

            @pl.when(z < nz - 1)
            def _():
                along_z(here(zz, x), zz, True).start()

            spread(here(zz, x), zz)

        @pl.when(z + s <= nz - 1)
        def _():
            zz = z + s
            along_z(here(zz, x), zz, False).wait_recv()

            @pl.when(z > 0)
            def _():
                along_z(here(zz, x), zz, False).start()

            spread(here(zz, x), zz)

    def x_one(zz):
        along_x(here(zz, left), zz, left, 0).wait_recv()
        half_on(zz, left, 0).start()
        across(here(zz, left), zz, left).start()
        along_x(here(zz, right), zz, right, 1).wait_recv()
        half_on(zz, right, 1).start()
        across(here(zz, right), zz, right).start()

    def h_one(zz):
        half_on(zz, far, 0).wait_recv()
        half_on(zz, far, 1).wait_recv()
        across(here(zz, far), zz, far).start()

    def both_ways(one, t):
        @pl.when(z - t >= 0)
        def _():
            one(z - t)

        @pl.when((t > 0) & (z + t <= nz - 1))
        def _():
            one(z + t)

    def step(s, _):
        @pl.when(s < nz)
        def _():
            z_stage(s)

        @pl.when(s <= nz)
        def _():
            both_ways(x_one, s - 1)

        @pl.when(s >= 2)
        def _():
            both_ways(h_one, s - 2)

        return 0

    lax.fori_loop(1, nz + 2, step, 0)

    def drain(zz, _):
        @pl.when((zz <= z) & (z < nz - 1))
        def _():
            along_z(here(zz, x), zz, True).wait_send()

        @pl.when((zz >= z) & (z > 0))
        def _():
            along_z(here(zz, x), zz, False).wait_send()

        for way in (0, 1):
            along_x(here(zz, x), zz, x, way).wait_send()
            half_on(zz, left if way == 0 else right, way).wait_send()
        for xx in range(nx):
            across(here(zz, xx), zz, xx).wait_send()
            at = zz * nx + xx
            other = out.at[slot(zz, xx, 1 - core)]
            remote(other, other, ps.at[at], pr.at[at], {CORE: 1 - core}).wait_recv()
        return 0

    lax.fori_loop(0, nz, drain, 0)
    own.wait()


def gathered(blk, nz, nx):
    shape = (nz * nx * 2, *blk.shape)
    return pl.pallas_call(
        functools.partial(gather_kernel, nz, nx),
        out_shape=jax.ShapeDtypeStruct(shape, blk.dtype),
        in_specs=[VMEM],
        out_specs=VMEM,
        scratch_shapes=[
            DMA((2, nz)),
            DMA((nz,)),
            DMA((2, nz)),
            DMA((2, nz)),
            DMA((2, nz)),
            DMA((2, nz)),
            DMA((nz * nx,)),
            DMA((nz * nx,)),
            DMA,
        ],
        compiler_params=pltpu.CompilerParams(
            collective_id=0, has_side_effects=True, vmem_limit_bytes=VMEM_LIMIT
        ),
        name="gather",
    )(blk)


def attend_kernel(
    group,
    head,
    half,
    scale,
    stash,
    ids,
    own_ids,
    queries,
    grads,
    blocks,
    dq,
    dkv,
    q_full,
    qs,
    gs,
    tops,
    totals,
    deltas,
    dq_sum,
    scores,
    dprobs,
    where_is,
    sem,
):
    total = ids.shape[0]
    per = 256 // half
    tiles = total // per
    rows = group * half
    fetch = pltpu.make_async_copy(queries.at[0, stash[0]], q_full, sem)
    fetch.start()

    def place(i, _):
        where_is[ids[i]] = i
        return 0

    lax.fori_loop(0, total, place, 0)
    low_first = (own_ids[0] < own_ids[1]).astype(jnp.int32)
    low = jnp.minimum(own_ids[0], own_ids[1])
    high = total - 1 - low
    halves = (low_first * half, (1 - low_first) * half)
    fetch.wait()
    for p in (0, 1):
        base = pl.multiple_of(halves[p], half)
        for h in range(group):
            cols = slice(h * head, (h + 1) * head)
            qs[p, h * half : (h + 1) * half, :] = q_full[pl.ds(base, half), cols]
            gs[p, h * half : (h + 1) * half, :] = grads[0, pl.ds(base, half), cols]
    tops[...] = jnp.full_like(tops, masked_score)
    totals[...] = jnp.zeros_like(totals)
    deltas[...] = jnp.zeros_like(deltas)
    dq_sum[...] = jnp.zeros_like(dq_sum)

    high_tiles = high // per + 1
    exp_scale = scale * math.log2(math.e)
    gap = lax.broadcasted_iota(jnp.int32, (256, rows), 0) - (
        lax.broadcasted_iota(jnp.int32, (256, rows), 1) % half
    )

    def unit(u):
        p = (u >= high_tiles).astype(jnp.int32)
        return p, u - p * high_tiles

    def tile_of(tile, first):
        pieces = []
        for i in range(per):
            at = where_is[tile * per + i]
            start = pl.multiple_of(first + (at % 2) * half, half)
            pieces.append(blocks[at // 2, pl.ds(start, half), :])
        return jnp.concatenate(pieces, axis=0)

    def cross(a, b, dims):
        return lax.dot_general(a, b, (dims, ((), ())), preferred_element_type=jnp.float32)

    def forward(u):
        p, tile = unit(u)
        mine = jnp.where(p == 0, high, low)
        t = cross(tile_of(tile, 0), qs[p], ((1,), (1,))) * exp_scale
        t = jnp.where(gap <= mine * half - tile * 256, t, masked_score)
        dprob = cross(tile_of(tile, 2 * half), gs[p], ((1,), (1,)))
        scores[u] = t
        dprobs[u] = dprob
        old = tops[p]
        new = jnp.maximum(old, jnp.max(t, axis=0, keepdims=True))
        fading = jnp.exp2(old - new)
        e = jnp.exp2(t - new)
        tops[p] = new
        totals[p] = totals[p] * fading + jnp.sum(e, axis=0, keepdims=True)
        deltas[p] = deltas[p] * fading + jnp.sum(e * dprob, axis=0, keepdims=True)

    units = tiles + 1
    together = 3 if units % 3 == 0 else 1

    def forward_step(i, _):
        for k in range(together):
            forward(i * together + k)
        return 0

    lax.fori_loop(0, units // together, forward_step, 0)
    deltas[...] = deltas[...] / totals[...]
    tops[...] = tops[...] + jnp.log2(totals[...])

    def backward(u):
        p, tile = unit(u)
        weights = jnp.exp2(scores[u] - tops[p])
        probs = weights.astype(jnp.bfloat16)
        dscore = (weights * (dprobs[u] - deltas[p]) * scale).astype(jnp.bfloat16)
        dk = cross(dscore, qs[p], ((1,), (0,)))
        dv = cross(probs, gs[p], ((1,), (0,)))
        dq_sum[p] += cross(tile_of(tile, 0), dscore, ((0,), (0,)))
        for i in range(per):
            at = where_is[tile * per + i]
            here = slice(i * half, (i + 1) * half)
            for part, first in ((dk, 0), (dv, 2 * half)):
                spot = (at // 2, pl.ds(pl.multiple_of(first + (at % 2) * half, half), half))
                before = jnp.where(p == 1, dkv[spot].astype(jnp.float32), 0.0)
                dkv[spot] = (before + part[here]).astype(jnp.bfloat16)

    def backward_step(i, _):
        for k in range(together):
            backward(i * together + k)
        return 0

    lax.fori_loop(0, units // together, backward_step, 0)

    def clear(s, _):
        at = where_is[s]
        for first in (0, 2 * half):
            spot = (at // 2, pl.ds(pl.multiple_of(first + (at % 2) * half, half), half))
            dkv[spot] = jnp.zeros((half, head), jnp.bfloat16)
        return 0

    lax.fori_loop(high_tiles * per, total, clear, 0)
    for p in (0, 1):
        base = pl.multiple_of(halves[p], half)
        turned = dq_sum[p].T.astype(jnp.bfloat16)
        for h in range(group):
            dq[pl.ds(base, half), h * head : (h + 1) * head] = turned[h * half : (h + 1) * half]


def attended(stash, ids, own_ids, queries, grads, blocks, head):
    tokens, width = queries.shape[2:]
    group, half = width // head, tokens // 2
    rows = group * half
    units = ids.shape[0] * half // 256 + 1
    return pl.pallas_call(
        functools.partial(attend_kernel, group, head, half, 1.0 / math.sqrt(head)),
        out_shape=(
            jax.ShapeDtypeStruct((tokens, width), jnp.bfloat16),
            jax.ShapeDtypeStruct((blocks.shape[0], 2 * tokens, head), jnp.bfloat16),
        ),
        in_specs=[SMEM, SMEM, SMEM, ANY, VMEM, VMEM],
        out_specs=(VMEM, VMEM),
        scratch_shapes=[
            pltpu.VMEM((tokens, width), jnp.bfloat16),
            pltpu.VMEM((2, rows, head), jnp.bfloat16),
            pltpu.VMEM((2, rows, head), jnp.bfloat16),
            pltpu.VMEM((2, 1, rows), jnp.float32),
            pltpu.VMEM((2, 1, rows), jnp.float32),
            pltpu.VMEM((2, 1, rows), jnp.float32),
            pltpu.VMEM((2, head, rows), jnp.float32),
            pltpu.VMEM((units, 256, rows), jnp.float32),
            pltpu.VMEM((units, 256, rows), jnp.float32),
            pltpu.SMEM((ids.shape[0],), jnp.int32),
            DMA,
        ],
        compiler_params=pltpu.CompilerParams(vmem_limit_bytes=VMEM_LIMIT),
        name="attend",
    )(stash, ids, own_ids, queries, grads, blocks)


def scatter_kernel(
    nz, nx, ns, dq, dkv, out, rx, held, hbuf, xbuf, zbuf, last, ps, pr, hs, hr, xs, xr, zs, zr, ms, mr
):
    z, x, core, right, left, far = neighbours(nz, nx)
    section = lax.axis_index(SECTION)
    ahead = lax.rem(section + ns - 1, ns)
    behind = lax.rem(section + 1, ns)
    tokens, width = dq.shape
    head = dkv.shape[2]
    ways = (right, left)

    barrier = pltpu.get_barrier_semaphore()
    pl.semaphore_signal(barrier, inc=1, device_id={SECTION: behind}, device_id_type=MESH)
    greet(nz, z, core, right, left, more=1)

    def pair(zz, xx):
        at = zz * nx + xx
        src = dkv.at[at * 2 + 1 - core]
        return remote(src, rx.at[at], ps.at[at], pr.at[at], {CORE: 1 - core})

    def nth(k):
        return jnp.where(k % 2 == 0, k // 2, nz - 1 - k // 2)

    main = remote(dq, out.at[:, pl.ds(0, width)], ms.at[0], mr.at[0], {SECTION: ahead})

    def launch(k, _):
        for xx in range(nx):
            pair(nth(k), xx).start()
        return 0

    lax.fori_loop(0, nz, launch, 0)
    main.start()

    def mine(zz, xx):
        at = zz * nx + xx
        return dkv[at * 2 + core].astype(jnp.float32) + rx[at].astype(jnp.float32)

    def half_on(zz, way):
        piece = held.at[zz, 0, pl.ds(way * tokens, tokens)]
        return remote(piece, hbuf.at[way, zz], hs.at[way, zz], hr.at[way, zz], {X: ways[way]})

    def along_x(zz, way):
        return remote(
            held.at[zz, 1 + way], xbuf.at[way, zz], xs.at[way, zz], xr.at[way, zz], {X: ways[way]}
        )

    def first(zz):
        for xx in range(nx):
            pair(zz, xx).wait_recv()
        held[zz, 0] = mine(zz, far).astype(jnp.bfloat16)
        half_on(zz, 0).start()
        half_on(zz, 1).start()

    def second(zz):
        for way in (0, 1):
            half_on(zz, way).wait_recv()
            own = mine(zz, ways[way])
            more = hbuf[way, zz].astype(jnp.float32)
            keep = (1 - way) * tokens
            joined = own[way * tokens : (way + 1) * tokens] + more
            held[zz, 1 + way, way * tokens : (way + 1) * tokens] = joined.astype(jnp.bfloat16)
            held[zz, 1 + way, keep : keep + tokens] = own[keep : keep + tokens].astype(jnp.bfloat16)
            along_x(zz, way).start()

    def third(zz):
        along_x(zz, 0).wait_recv()
        along_x(zz, 1).wait_recv()
        done = mine(zz, x) + xbuf[0, zz].astype(jnp.float32) + xbuf[1, zz].astype(jnp.float32)
        held[zz, 3] = done.astype(jnp.bfloat16)

    pieces = (pl.ds(0, tokens), pl.ds(tokens, tokens))

    def along_z(zz, down, piece):
        to = z - 1 if down else z + 1
        way = 0 if down else 1
        return remote(
            held.at[zz, 3, pieces[piece]],
            zbuf.at[way, zz, pieces[piece]],
            zs.at[way, zz, piece],
            zr.at[way, zz, piece],
            {Z: to},
        )

    def chain(zz, down, source):
        way = 0 if down else 1
        for piece in (0, 1):

            @pl.when(source)
            def _():
                along_z(zz, down, piece).wait_recv()
                joined = held[zz, 3, pieces[piece]].astype(jnp.float32) + zbuf[
                    way, zz, pieces[piece]
                ].astype(jnp.float32)
                held[zz, 3, pieces[piece]] = joined.astype(jnp.bfloat16)

            along_z(zz, down, piece).start()

    def up_chain(t):
        i = t - z

        @pl.when((i >= 0) & (i < nz - 1 - z))
        def _():
            chain(nz - 1 - i, False, z > 0)

    def down_chain(t):
        i = t - (nz - 1 - z)

        @pl.when((i >= 0) & (i < z))
        def _():
            chain(i, True, z < nz - 1)

    def step(k, _):
        @pl.when(k < nz)
        def _():
            first(nth(k))

        @pl.when((k >= 1) & (k <= nz))
        def _():
            second(nth(k - 1))

        @pl.when((k >= 2) & (k <= nz + 1))
        def _():
            third(nth(k - 2))

        @pl.when((k >= 3) & ((k % 2 == 1) | (k > nz + 1)))
        def _():
            t = jnp.where(k > nz + 1, k - (nz + 2) + nz // 2, (k - 3) // 2)
            up_chain(t)
            down_chain(t)

        return 0

    lax.fori_loop(0, nz + 2 + nz - 1 - nz // 2, step, 0)

    for piece in (0, 1):
        last[pieces[piece]] = held[z, 3, pieces[piece]].astype(jnp.float32)

        @pl.when(z < nz - 1)
        def _():
            along_z(z, True, piece).wait_recv()
            last[pieces[piece]] += zbuf[0, z, pieces[piece]].astype(jnp.float32)

        @pl.when(z > 0)
        def _():
            along_z(z, False, piece).wait_recv()
            last[pieces[piece]] += zbuf[1, z, pieces[piece]].astype(jnp.float32)

        held[z, 3, pieces[piece]] = last[pieces[piece]].astype(jnp.bfloat16)

    def tail(piece):
        return remote(
            held.at[z, 3, pieces[piece]],
            out.at[:, pl.ds(width + piece * head, head)],
            ms.at[1 + piece],
            mr.at[1 + piece],
            {SECTION: ahead},
        )

    for piece in (0, 1):
        tail(piece).start()

    def drain(zz, _):
        for xx in range(nx):
            pair(zz, xx).wait_send()
        for way in (0, 1):
            half_on(zz, way).wait_send()
            along_x(zz, way).wait_send()
        for piece in (0, 1):

            @pl.when(zz < z)
            def _():
                along_z(zz, True, piece).wait_send()

            @pl.when(zz > z)
            def _():
                along_z(zz, False, piece).wait_send()

        return 0

    lax.fori_loop(0, nz, drain, 0)
    main.wait()
    for piece in (0, 1):
        tail(piece).wait()


def scattered(dq, dkv, nz, nx, ns):
    tokens, width = dq.shape
    rows, head = dkv.shape[1:]
    half = jnp.bfloat16
    return pl.pallas_call(
        functools.partial(scatter_kernel, nz, nx, ns),
        out_shape=jax.ShapeDtypeStruct((tokens, width + 2 * head), half),
        in_specs=[VMEM, VMEM],
        out_specs=VMEM,
        scratch_shapes=[
            pltpu.VMEM((nz * nx, rows, head), half),
            pltpu.VMEM((nz, 4, rows, head), half),
            pltpu.VMEM((2, nz, rows // 2, head), half),
            pltpu.VMEM((2, nz, rows, head), half),
            pltpu.VMEM((2, nz, rows, head), half),
            pltpu.VMEM((rows, head), jnp.float32),
            DMA((nz * nx,)),
            DMA((nz * nx,)),
            DMA((2, nz)),
            DMA((2, nz)),
            DMA((2, nz)),
            DMA((2, nz)),
            DMA((2, nz, 2)),
            DMA((2, nz, 2)),
            DMA((3,)),
            DMA((3,)),
        ],
        compiler_params=pltpu.CompilerParams(
            collective_id=1, has_side_effects=True, vmem_limit_bytes=VMEM_LIMIT
        ),
        name="scatter",
    )(dq, dkv)


def per_device(sizes, queries, keys, values, out_grad, stretch_ids, stash_slot):
    ns, nz, nx = sizes
    stash_index = stash_slot[0]
    key_rows = lax.dynamic_index_in_dim(keys[0], stash_index, 0, keepdims=False)
    value_rows = lax.dynamic_index_in_dim(values[0], stash_index, 0, keepdims=False)
    head = key_rows.shape[1]
    lane = lax.broadcasted_iota(jnp.int32, (ID_ROWS, head), 1)
    id_rows = jnp.where(lane < head // 2, stretch_ids[0], stretch_ids[1]).astype(jnp.bfloat16)
    blk = jnp.concatenate([key_rows, value_rows, id_rows], axis=0)
    blocks = gathered(blk, nz, nx)
    ids = blocks[:, 2 * key_rows.shape[0], :: head // 2].astype(jnp.int32).reshape(-1)
    dq, dkv = attended(stash_slot, ids, stretch_ids, queries, out_grad, blocks, head)
    return scattered(dq, dkv, nz, nx, ns)[None]


def solution(mesh):
    ns = mesh.shape["section"]
    nz, nx = 8, 4
    split = Mesh(mesh.devices.reshape(ns, nz, nx, 2), (SECTION, Z, X, CORE))
    return jax.shard_map(
        functools.partial(per_device, (ns, nz, nx)),
        mesh=split,
        in_specs=(
            P(SECTION, None, CTX, None),
            P(SECTION, None, CTX, None),
            P(SECTION, None, CTX, None),
            P(SECTION, CTX, None),
            P(CTX),
            P(SECTION),
        ),
        out_specs=P(SECTION, CTX, None),
        check_vma=False,
    )
```

```python
import functools
import math

import jax
import jax.numpy as jnp
from jax import lax
from jax.experimental import pallas as pl
from jax.experimental.pallas import tpu as pltpu
from jax.sharding import Mesh
from jax.sharding import PartitionSpec as P

Z, X, CORE, SECTION = "ctx_0", "ctx_1", "ctx_2", "section"
CTX = (Z, X, CORE)
MESH = pl.DeviceIdType.MESH
VMEM = pl.BlockSpec(memory_space=pltpu.VMEM)
SMEM = pl.BlockSpec(memory_space=pltpu.SMEM)
ANY = pl.BlockSpec(memory_space=pl.ANY)
IN_HBM = pl.BlockSpec(memory_space=pltpu.HBM)
DMA = pltpu.SemaphoreType.DMA
VMEM_LIMIT = 60 * 1024 * 1024

ID_ROWS = 16
PIECES = 2
masked_score = -1e30


def neighbours(nz, nx):
    z, x, core = lax.axis_index(Z), lax.axis_index(X), lax.axis_index(CORE)
    right = lax.rem(x + 1, nx)
    left = lax.rem(x + nx - 1, nx)
    far = lax.rem(x + nx // 2, nx)
    return z, x, core, right, left, far


def greet(nz, z, core, right, left, more=0):
    barrier = pltpu.get_barrier_semaphore()

    def signal(**where):
        pl.semaphore_signal(barrier, inc=1, device_id=dict(where), device_id_type=MESH)

    signal(**{X: right})
    signal(**{X: left})
    signal(**{CORE: 1 - core})

    @pl.when(z > 0)
    def _():
        signal(**{Z: z - 1})

    @pl.when(z < nz - 1)
    def _():
        signal(**{Z: z + 1})

    inside = (z > 0).astype(jnp.int32) + (z < nz - 1).astype(jnp.int32)
    pl.semaphore_wait(barrier, 3 + more + inside)


def remote(src, dst, send, recv, where):
    return pltpu.make_async_remote_copy(
        src_ref=src, dst_ref=dst, send_sem=send, recv_sem=recv, device_id=where, device_id_type=MESH
    )


def gather_kernel(nz, nx, blk, out, zs, zr, xs, xr, hs, hr, ps, pr, own_sem):
    z, x, core, right, left, far = neighbours(nz, nx)
    rows = blk.shape[0]
    cut = rows // 2 // 16 * 16
    halves = (pl.ds(0, cut), pl.ds(cut, rows - cut))
    size = rows // PIECES // 16 * 16
    pieces = [pl.ds(i * size, size if i < PIECES - 1 else rows - i * size) for i in range(PIECES)]

    def slot(zz, xx, cc):
        return (zz * nx + xx) * 2 + cc

    own = pltpu.make_async_copy(blk, out.at[slot(z, x, core)], own_sem)
    own.start()
    greet(nz, z, core, right, left)

    def along_z(src, zz, up, i):
        to = z + 1 if up else z - 1
        return remote(
            src.at[pieces[i]],
            out.at[slot(zz, x, core), pieces[i]],
            zs.at[0 if up else 1, zz, i],
            zr.at[zz, i],
            {Z: to},
        )

    def along_x(src, zz, xx, way):
        to = right if way == 0 else left
        return remote(src, out.at[slot(zz, xx, core)], xs.at[way, zz], xr.at[way, zz], {X: to})

    def half_on(zz, xx, way):
        to = right if way == 0 else left
        piece = out.at[slot(zz, xx, core), halves[way]]
        return remote(piece, piece, hs.at[way, zz], hr.at[way, zz], {X: to})

    def across(src, zz, xx):
        at = zz * nx + xx
        return remote(src, out.at[slot(zz, xx, core)], ps.at[at], pr.at[at], {CORE: 1 - core})

    def here(zz, xx):
        return out.at[slot(zz, xx, core)]

    def spread(src, zz):
        along_x(src, zz, x, 0).start()
        along_x(src, zz, x, 1).start()
        across(src, zz, x).start()

    @pl.when(z < nz - 1)
    def _():
        for i in range(PIECES):
            along_z(blk, z, True, i).start()

    @pl.when(z > 0)
    def _():
        for i in range(PIECES):
            along_z(blk, z, False, i).start()

    spread(blk, z)

    def z_stage(s):
        @pl.when(z - s >= 0)
        def _():
            zz = z - s
            for i in range(PIECES):
                along_z(here(zz, x), zz, True, i).wait_recv()

                @pl.when(z < nz - 1)
                def _():
                    along_z(here(zz, x), zz, True, i).start()

            spread(here(zz, x), zz)

        @pl.when(z + s <= nz - 1)
        def _():
            zz = z + s
            for i in range(PIECES):
                along_z(here(zz, x), zz, False, i).wait_recv()

                @pl.when(z > 0)
                def _():
                    along_z(here(zz, x), zz, False, i).start()

            spread(here(zz, x), zz)

    def x_one(zz):
        along_x(here(zz, left), zz, left, 0).wait_recv()
        half_on(zz, left, 0).start()
        across(here(zz, left), zz, left).start()
        along_x(here(zz, right), zz, right, 1).wait_recv()
        half_on(zz, right, 1).start()
        across(here(zz, right), zz, right).start()

    def h_one(zz):
        half_on(zz, far, 0).wait_recv()
        half_on(zz, far, 1).wait_recv()
        across(here(zz, far), zz, far).start()

    def both_ways(one, t):
        @pl.when(z - t >= 0)
        def _():
            one(z - t)

        @pl.when((t > 0) & (z + t <= nz - 1))
        def _():
            one(z + t)

    def step(s, _):
        @pl.when(s < nz)
        def _():
            z_stage(s)

        @pl.when(s <= nz)
        def _():
            both_ways(x_one, s - 1)

        @pl.when(s >= 2)
        def _():
            both_ways(h_one, s - 2)

        return 0

    lax.fori_loop(1, nz + 2, step, 0)

    def drain(zz, _):
        @pl.when((zz <= z) & (z < nz - 1))
        def _():
            for i in range(PIECES):
                along_z(here(zz, x), zz, True, i).wait_send()

        @pl.when((zz >= z) & (z > 0))
        def _():
            for i in range(PIECES):
                along_z(here(zz, x), zz, False, i).wait_send()

        for way in (0, 1):
            along_x(here(zz, x), zz, x, way).wait_send()
            half_on(zz, left if way == 0 else right, way).wait_send()
        for xx in range(nx):
            across(here(zz, xx), zz, xx).wait_send()
            at = zz * nx + xx
            other = out.at[slot(zz, xx, 1 - core)]
            remote(other, other, ps.at[at], pr.at[at], {CORE: 1 - core}).wait_recv()
        return 0

    lax.fori_loop(0, nz, drain, 0)
    own.wait()


def gathered(blk, nz, nx):
    shape = (nz * nx * 2, *blk.shape)
    return pl.pallas_call(
        functools.partial(gather_kernel, nz, nx),
        out_shape=jax.ShapeDtypeStruct(shape, blk.dtype),
        in_specs=[VMEM],
        out_specs=VMEM,
        scratch_shapes=[
            DMA((2, nz, PIECES)),
            DMA((nz, PIECES)),
            DMA((2, nz)),
            DMA((2, nz)),
            DMA((2, nz)),
            DMA((2, nz)),
            DMA((nz * nx,)),
            DMA((nz * nx,)),
            DMA,
        ],
        compiler_params=pltpu.CompilerParams(
            collective_id=0, has_side_effects=True, vmem_limit_bytes=8 * 1024 * 1024
        ),
        name="gather",
    )(blk)


def attend_kernel(
    group,
    head,
    half,
    scale,
    stash,
    own_ids,
    queries,
    grads,
    blocks,
    dq,
    dkv,
    q_full,
    qs,
    gs,
    tops,
    totals,
    deltas,
    dq_sum,
    scores,
    dprobs,
    where_is,
    id_rows,
    ids,
    sems,
):
    total = 2 * blocks.shape[0]
    per = 256 // half
    tiles = total // per
    rows = group * half
    fetch = pltpu.make_async_copy(queries.at[0, stash[0]], q_full, sems.at[0])
    fetch.start()

    numbers = blocks[:, 4 * half :, :].astype(jnp.float32)
    id_rows[...] = jnp.max(numbers, axis=1).astype(jnp.int32)
    listing = pltpu.make_async_copy(id_rows, ids, sems.at[1])
    listing.start()
    low_first = (own_ids[0] < own_ids[1]).astype(jnp.int32)
    low = jnp.minimum(own_ids[0], own_ids[1])
    high = total - 1 - low
    halves = (low_first * half, (1 - low_first) * half)
    fetch.wait()
    for p in (0, 1):
        base = pl.multiple_of(halves[p], half)
        for h in range(group):
            cols = slice(h * head, (h + 1) * head)
            qs[p, h * half : (h + 1) * half, :] = q_full[pl.ds(base, half), cols]
            gs[p, h * half : (h + 1) * half, :] = grads[0, pl.ds(base, half), cols]
    tops[...] = jnp.full_like(tops, masked_score)
    totals[...] = jnp.zeros_like(totals)
    deltas[...] = jnp.zeros_like(deltas)
    dq_sum[...] = jnp.zeros_like(dq_sum)

    listing.wait()

    def place(i, _):
        where_is[ids[i, 0]] = 2 * i
        where_is[ids[i, head // 2]] = 2 * i + 1
        return 0

    lax.fori_loop(0, total // 2, place, 0)
    high_tiles = high // per + 1
    exp_scale = scale * math.log2(math.e)
    gap = lax.broadcasted_iota(jnp.int32, (256, rows), 0) - (
        lax.broadcasted_iota(jnp.int32, (256, rows), 1) % half
    )

    def unit(u):
        p = (u >= high_tiles).astype(jnp.int32)
        return p, u - p * high_tiles

    def tile_of(tile, first):
        pieces = []
        for i in range(per):
            at = where_is[tile * per + i]
            start = pl.multiple_of(first + (at % 2) * half, half)
            pieces.append(blocks[at // 2, pl.ds(start, half), :])
        return jnp.concatenate(pieces, axis=0)

    def cross(a, b, dims):
        return lax.dot_general(a, b, (dims, ((), ())), preferred_element_type=jnp.float32)

    def forward(u):
        p, tile = unit(u)
        mine = jnp.where(p == 0, high, low)
        t = cross(tile_of(tile, 0), qs[p], ((1,), (1,))) * exp_scale
        t = jnp.where(gap <= mine * half - tile * 256, t, masked_score)
        dprob = cross(tile_of(tile, 2 * half), gs[p], ((1,), (1,)))
        scores[u] = t
        dprobs[u] = dprob
        old = tops[p]
        new = jnp.maximum(old, jnp.max(t, axis=0, keepdims=True))
        fading = jnp.exp2(old - new)
        e = jnp.exp2(t - new)
        tops[p] = new
        totals[p] = totals[p] * fading + jnp.sum(e, axis=0, keepdims=True)
        deltas[p] = deltas[p] * fading + jnp.sum(e * dprob, axis=0, keepdims=True)

    units = tiles + 1
    together = 3 if units % 3 == 0 else 1

    def forward_step(i, _):
        for k in range(together):
            forward(i * together + k)
        return 0

    lax.fori_loop(0, units // together, forward_step, 0)
    deltas[...] = deltas[...] / totals[...]
    tops[...] = tops[...] + jnp.log2(totals[...])

    def backward(u):
        p, tile = unit(u)
        weights = jnp.exp2(scores[u] - tops[p])
        probs = weights.astype(jnp.bfloat16)
        dscore = (weights * (dprobs[u] - deltas[p]) * scale).astype(jnp.bfloat16)
        dk = cross(dscore, qs[p], ((1,), (0,)))
        dv = cross(probs, gs[p], ((1,), (0,)))
        dq_sum[p] += cross(tile_of(tile, 0), dscore, ((0,), (0,)))
        for i in range(per):
            at = where_is[tile * per + i]
            here = slice(i * half, (i + 1) * half)
            for part, first in ((dk, 0), (dv, 2 * half)):
                spot = (at // 2, pl.ds(pl.multiple_of(first + (at % 2) * half, half), half))
                before = jnp.where(p == 1, dkv[spot].astype(jnp.float32), 0.0)
                dkv[spot] = (before + part[here]).astype(jnp.bfloat16)

    def backward_step(i, _):
        for k in range(together):
            backward(i * together + k)
        return 0

    lax.fori_loop(0, units // together, backward_step, 0)

    def clear(s, _):
        at = where_is[s]
        for first in (0, 2 * half):
            spot = (at // 2, pl.ds(pl.multiple_of(first + (at % 2) * half, half), half))
            dkv[spot] = jnp.zeros((half, head), jnp.bfloat16)
        return 0

    lax.fori_loop(high_tiles * per, total, clear, 0)
    for p in (0, 1):
        base = pl.multiple_of(halves[p], half)
        turned = dq_sum[p].T.astype(jnp.bfloat16)
        for h in range(group):
            dq[pl.ds(base, half), h * head : (h + 1) * head] = turned[h * half : (h + 1) * half]


def attended(stash, own_ids, queries, grads, blocks, head):
    tokens, width = queries.shape[2:]
    group, half = width // head, tokens // 2
    rows = group * half
    total = 2 * blocks.shape[0]
    units = total * half // 256 + 1
    return pl.pallas_call(
        functools.partial(attend_kernel, group, head, half, 1.0 / math.sqrt(head)),
        out_shape=(
            jax.ShapeDtypeStruct((tokens, width), jnp.bfloat16),
            jax.ShapeDtypeStruct((blocks.shape[0], 2 * tokens, head), jnp.bfloat16),
        ),
        in_specs=[SMEM, SMEM, ANY, VMEM, VMEM],
        out_specs=(VMEM, VMEM),
        scratch_shapes=[
            pltpu.VMEM((tokens, width), jnp.bfloat16),
            pltpu.VMEM((2, rows, head), jnp.bfloat16),
            pltpu.VMEM((2, rows, head), jnp.bfloat16),
            pltpu.VMEM((2, 1, rows), jnp.float32),
            pltpu.VMEM((2, 1, rows), jnp.float32),
            pltpu.VMEM((2, 1, rows), jnp.float32),
            pltpu.VMEM((2, head, rows), jnp.float32),
            pltpu.VMEM((units, 256, rows), jnp.float32),
            pltpu.VMEM((units, 256, rows), jnp.float32),
            pltpu.SMEM((total,), jnp.int32),
            pltpu.VMEM((total // 2, head), jnp.int32),
            pltpu.SMEM((total // 2, head), jnp.int32),
            DMA((2,)),
        ],
        compiler_params=pltpu.CompilerParams(vmem_limit_bytes=32 * 1024 * 1024),
        name="attend",
    )(stash, own_ids, queries, grads, blocks)


def scatter_kernel(
    nz, nx, ns, dq, dkv, out, rx, held, hbuf, xbuf, zbuf, last, ps, pr, hs, hr, xs, xr, zs, zr, ms, mr
):
    z, x, core, right, left, far = neighbours(nz, nx)
    section = lax.axis_index(SECTION)
    ahead = lax.rem(section + ns - 1, ns)
    behind = lax.rem(section + 1, ns)
    tokens, width = dq.shape
    head = dkv.shape[2]
    ways = (right, left)

    barrier = pltpu.get_barrier_semaphore()
    pl.semaphore_signal(barrier, inc=1, device_id={SECTION: behind}, device_id_type=MESH)
    greet(nz, z, core, right, left, more=1)

    def pair(zz, xx):
        at = zz * nx + xx
        src = dkv.at[at * 2 + 1 - core]
        return remote(src, rx.at[at], ps.at[at], pr.at[at], {CORE: 1 - core})

    def nth(k):
        return jnp.where(k % 2 == 0, k // 2, nz - 1 - k // 2)

    main = remote(dq, out.at[:, pl.ds(0, width)], ms.at[0], mr.at[0], {SECTION: ahead})

    main.start()

    def launch(k, _):
        for xx in range(nx):
            pair(nth(k), xx).start()
        return 0

    lax.fori_loop(0, nz, launch, 0)

    def mine(zz, xx):
        at = zz * nx + xx
        return dkv[at * 2 + core].astype(jnp.float32) + rx[at].astype(jnp.float32)

    def half_on(zz, way):
        piece = held.at[zz, 0, pl.ds(way * tokens, tokens)]
        return remote(piece, hbuf.at[way, zz], hs.at[way, zz], hr.at[way, zz], {X: ways[way]})

    def along_x(zz, way):
        return remote(
            held.at[zz, 1 + way], xbuf.at[way, zz], xs.at[way, zz], xr.at[way, zz], {X: ways[way]}
        )

    def first(zz):
        for xx in range(nx):
            pair(zz, xx).wait_recv()
        held[zz, 0] = mine(zz, far).astype(jnp.bfloat16)
        half_on(zz, 0).start()
        half_on(zz, 1).start()

    def second(zz):
        for way in (0, 1):
            half_on(zz, way).wait_recv()
            own = mine(zz, ways[way])
            more = hbuf[way, zz].astype(jnp.float32)
            keep = (1 - way) * tokens
            joined = own[way * tokens : (way + 1) * tokens] + more
            held[zz, 1 + way, way * tokens : (way + 1) * tokens] = joined.astype(jnp.bfloat16)
            held[zz, 1 + way, keep : keep + tokens] = own[keep : keep + tokens].astype(jnp.bfloat16)
            along_x(zz, way).start()

    def third(zz):
        along_x(zz, 0).wait_recv()
        along_x(zz, 1).wait_recv()
        done = mine(zz, x) + xbuf[0, zz].astype(jnp.float32) + xbuf[1, zz].astype(jnp.float32)
        held[zz, 3] = done.astype(jnp.bfloat16)

    pieces = (pl.ds(0, tokens), pl.ds(tokens, tokens))

    def along_z(zz, down, piece):
        to = z - 1 if down else z + 1
        way = 0 if down else 1
        return remote(
            held.at[zz, 3, pieces[piece]],
            zbuf.at[way, zz, pieces[piece]],
            zs.at[way, zz, piece],
            zr.at[way, zz, piece],
            {Z: to},
        )

    def chain(zz, down, source):
        way = 0 if down else 1
        for piece in (0, 1):

            @pl.when(source)
            def _():
                along_z(zz, down, piece).wait_recv()
                joined = held[zz, 3, pieces[piece]].astype(jnp.float32) + zbuf[
                    way, zz, pieces[piece]
                ].astype(jnp.float32)
                held[zz, 3, pieces[piece]] = joined.astype(jnp.bfloat16)

            along_z(zz, down, piece).start()

    def up_chain(t):
        i = t - z

        @pl.when((i >= 0) & (i < nz - 1 - z))
        def _():
            chain(nz - 1 - i, False, z > 0)

    def down_chain(t):
        i = t - (nz - 1 - z)

        @pl.when((i >= 0) & (i < z))
        def _():
            chain(i, True, z < nz - 1)

    def step(k, _):
        @pl.when(k < nz)
        def _():
            first(nth(k))

        @pl.when((k >= 1) & (k <= nz))
        def _():
            second(nth(k - 1))

        @pl.when((k >= 2) & (k <= nz + 1))
        def _():
            third(nth(k - 2))

        @pl.when((k >= 3) & ((k % 2 == 1) | (k > nz + 1)))
        def _():
            t = jnp.where(k > nz + 1, k - (nz + 2) + nz // 2, (k - 3) // 2)
            up_chain(t)
            down_chain(t)

        return 0

    lax.fori_loop(0, nz + 2 + nz - 1 - nz // 2, step, 0)

    def tail(piece):
        return remote(
            held.at[z, 3, pieces[piece]],
            out.at[:, pl.ds(width + piece * head, head)],
            ms.at[1 + piece],
            mr.at[1 + piece],
            {SECTION: ahead},
        )

    for piece in (0, 1):
        last[pieces[piece]] = held[z, 3, pieces[piece]].astype(jnp.float32)

        @pl.when(z < nz - 1)
        def _():
            along_z(z, True, piece).wait_recv()
            last[pieces[piece]] += zbuf[0, z, pieces[piece]].astype(jnp.float32)

        @pl.when(z > 0)
        def _():
            along_z(z, False, piece).wait_recv()
            last[pieces[piece]] += zbuf[1, z, pieces[piece]].astype(jnp.float32)

        held[z, 3, pieces[piece]] = last[pieces[piece]].astype(jnp.bfloat16)
        tail(piece).start()

    def drain(zz, _):
        for xx in range(nx):
            pair(zz, xx).wait_send()
        for way in (0, 1):
            half_on(zz, way).wait_send()
            along_x(zz, way).wait_send()
        for piece in (0, 1):

            @pl.when(zz < z)
            def _():
                along_z(zz, True, piece).wait_send()

            @pl.when(zz > z)
            def _():
                along_z(zz, False, piece).wait_send()

        return 0

    lax.fori_loop(0, nz, drain, 0)
    main.wait()
    for piece in (0, 1):
        tail(piece).wait()


def scattered(dq, dkv, nz, nx, ns):
    tokens, width = dq.shape
    rows, head = dkv.shape[1:]
    half = jnp.bfloat16
    return pl.pallas_call(
        functools.partial(scatter_kernel, nz, nx, ns),
        out_shape=jax.ShapeDtypeStruct((tokens, width + 2 * head), half),
        in_specs=[VMEM, VMEM],
        out_specs=VMEM,
        scratch_shapes=[
            pltpu.VMEM((nz * nx, rows, head), half),
            pltpu.VMEM((nz, 4, rows, head), half),
            pltpu.VMEM((2, nz, rows // 2, head), half),
            pltpu.VMEM((2, nz, rows, head), half),
            pltpu.VMEM((2, nz, rows, head), half),
            pltpu.VMEM((rows, head), jnp.float32),
            DMA((nz * nx,)),
            DMA((nz * nx,)),
            DMA((2, nz)),
            DMA((2, nz)),
            DMA((2, nz)),
            DMA((2, nz)),
            DMA((2, nz, 2)),
            DMA((2, nz, 2)),
            DMA((3,)),
            DMA((3,)),
        ],
        compiler_params=pltpu.CompilerParams(
            collective_id=1, has_side_effects=True, vmem_limit_bytes=16 * 1024 * 1024
        ),
        name="scatter",
    )(dq, dkv)


def pack_kernel(stash, own_ids, keys, values, blk, sems):
    rows = keys.shape[2]
    parts = []
    for i, source in enumerate((keys, values)):
        part = pltpu.make_async_copy(
            source.at[0, stash[0]], blk.at[pl.ds(i * rows, rows)], sems.at[i]
        )
        part.start()
        parts.append(part)
    lane = lax.broadcasted_iota(jnp.int32, (ID_ROWS, blk.shape[1]), 1)
    numbers = jnp.where(lane < blk.shape[1] // 2, own_ids[0], own_ids[1])
    blk[2 * rows :, :] = numbers.astype(jnp.float32).astype(jnp.bfloat16)
    for part in parts:
        part.wait()


def packed(stash, own_ids, keys, values):
    rows, head = keys.shape[2:]
    return pl.pallas_call(
        pack_kernel,
        out_shape=jax.ShapeDtypeStruct((2 * rows + ID_ROWS, head), keys.dtype),
        in_specs=[SMEM, SMEM, IN_HBM, IN_HBM],
        out_specs=VMEM,
        scratch_shapes=[DMA((2,))],
        compiler_params=pltpu.CompilerParams(vmem_limit_bytes=4 * 1024 * 1024),
        name="pack",
    )(stash, own_ids, keys, values)


def per_device(sizes, queries, keys, values, out_grad, stretch_ids, stash_slot):
    ns, nz, nx = sizes
    head = keys.shape[3]
    blk = packed(stash_slot, stretch_ids, keys, values)
    blocks = gathered(blk, nz, nx)
    dq, dkv = attended(stash_slot, stretch_ids, queries, out_grad, blocks, head)
    return scattered(dq, dkv, nz, nx, ns)[None]


def solution(mesh):
    ns = mesh.shape["section"]
    nz, nx = 8, 4
    split = Mesh(mesh.devices.reshape(ns, nz, nx, 2), (SECTION, Z, X, CORE))
    return jax.shard_map(
        functools.partial(per_device, (ns, nz, nx)),
        mesh=split,
        in_specs=(
            P(SECTION, None, CTX, None),
            P(SECTION, None, CTX, None),
            P(SECTION, None, CTX, None),
            P(SECTION, CTX, None),
            P(CTX),
            P(SECTION),
        ),
        out_specs=P(SECTION, CTX, None),
        check_vma=False,
    )
```

```python
import functools
import math

import jax
import jax.numpy as jnp
from jax import lax
from jax.experimental import pallas as pl
from jax.experimental.pallas import tpu as pltpu
from jax.sharding import Mesh
from jax.sharding import PartitionSpec as P

Z, X, CORE, SECTION = "ctx_0", "ctx_1", "ctx_2", "section"
CTX = (Z, X, CORE)
MESH = pl.DeviceIdType.MESH
VMEM = pl.BlockSpec(memory_space=pltpu.VMEM)
SMEM = pl.BlockSpec(memory_space=pltpu.SMEM)
ANY = pl.BlockSpec(memory_space=pl.ANY)
IN_HBM = pl.BlockSpec(memory_space=pltpu.HBM)
DMA = pltpu.SemaphoreType.DMA
VMEM_LIMIT = 60 * 1024 * 1024

ID_ROWS = 16
PIECES = 2
masked_score = -1e30


def neighbours(nz, nx):
    z, x, core = lax.axis_index(Z), lax.axis_index(X), lax.axis_index(CORE)
    right = lax.rem(x + 1, nx)
    left = lax.rem(x + nx - 1, nx)
    far = lax.rem(x + nx // 2, nx)
    return z, x, core, right, left, far


def greet(nz, z, core, right, left, more=0):
    barrier = pltpu.get_barrier_semaphore()

    def signal(**where):
        pl.semaphore_signal(barrier, inc=1, device_id=dict(where), device_id_type=MESH)

    signal(**{X: right})
    signal(**{X: left})
    signal(**{CORE: 1 - core})

    @pl.when(z > 0)
    def _():
        signal(**{Z: z - 1})

    @pl.when(z < nz - 1)
    def _():
        signal(**{Z: z + 1})

    inside = (z > 0).astype(jnp.int32) + (z < nz - 1).astype(jnp.int32)
    pl.semaphore_wait(barrier, 3 + more + inside)


def remote(src, dst, send, recv, where):
    return pltpu.make_async_remote_copy(
        src_ref=src, dst_ref=dst, send_sem=send, recv_sem=recv, device_id=where, device_id_type=MESH
    )


def gather_kernel(nz, nx, blk, out, zs, zr, xs, xr, hs, hr, ps, pr, own_sem):
    z, x, core, right, left, far = neighbours(nz, nx)
    rows = blk.shape[0]
    cut = rows // 2 // 16 * 16
    halves = (pl.ds(0, cut), pl.ds(cut, rows - cut))
    size = rows // PIECES // 16 * 16
    pieces = [pl.ds(i * size, size if i < PIECES - 1 else rows - i * size) for i in range(PIECES)]

    def slot(zz, xx, cc):
        return (zz * nx + xx) * 2 + cc

    own = pltpu.make_async_copy(blk, out.at[slot(z, x, core)], own_sem)
    own.start()
    greet(nz, z, core, right, left)

    def along_z(src, zz, up, i):
        to = z + 1 if up else z - 1
        return remote(
            src.at[pieces[i]],
            out.at[slot(zz, x, core), pieces[i]],
            zs.at[0 if up else 1, zz, i],
            zr.at[zz, i],
            {Z: to},
        )

    def along_x(src, zz, xx, way):
        to = right if way == 0 else left
        return remote(src, out.at[slot(zz, xx, core)], xs.at[way, zz], xr.at[way, zz], {X: to})

    def half_on(zz, xx, way):
        to = right if way == 0 else left
        piece = out.at[slot(zz, xx, core), halves[way]]
        return remote(piece, piece, hs.at[way, zz], hr.at[way, zz], {X: to})

    def across(src, zz, xx):
        at = zz * nx + xx
        return remote(src, out.at[slot(zz, xx, core)], ps.at[at], pr.at[at], {CORE: 1 - core})

    def here(zz, xx):
        return out.at[slot(zz, xx, core)]

    def spread(src, zz):
        along_x(src, zz, x, 0).start()
        along_x(src, zz, x, 1).start()
        across(src, zz, x).start()

    @pl.when(z < nz - 1)
    def _():
        for i in range(PIECES):
            along_z(blk, z, True, i).start()

    @pl.when(z > 0)
    def _():
        for i in range(PIECES):
            along_z(blk, z, False, i).start()

    spread(blk, z)

    def z_stage(s):
        @pl.when(z - s >= 0)
        def _():
            zz = z - s
            for i in range(PIECES):
                along_z(here(zz, x), zz, True, i).wait_recv()

                @pl.when(z < nz - 1)
                def _():
                    along_z(here(zz, x), zz, True, i).start()

            spread(here(zz, x), zz)

        @pl.when(z + s <= nz - 1)
        def _():
            zz = z + s
            for i in range(PIECES):
                along_z(here(zz, x), zz, False, i).wait_recv()

                @pl.when(z > 0)
                def _():
                    along_z(here(zz, x), zz, False, i).start()

            spread(here(zz, x), zz)

    def x_one(zz):
        along_x(here(zz, left), zz, left, 0).wait_recv()
        half_on(zz, left, 0).start()
        across(here(zz, left), zz, left).start()
        along_x(here(zz, right), zz, right, 1).wait_recv()
        half_on(zz, right, 1).start()
        across(here(zz, right), zz, right).start()

    def h_one(zz):
        half_on(zz, far, 0).wait_recv()
        half_on(zz, far, 1).wait_recv()
        across(here(zz, far), zz, far).start()

    def both_ways(one, t):
        @pl.when(z - t >= 0)
        def _():
            one(z - t)

        @pl.when((t > 0) & (z + t <= nz - 1))
        def _():
            one(z + t)

    def step(s, _):
        @pl.when(s < nz)
        def _():
            z_stage(s)

        @pl.when(s <= nz)
        def _():
            both_ways(x_one, s - 1)

        @pl.when(s >= 2)
        def _():
            both_ways(h_one, s - 2)

        return 0

    lax.fori_loop(1, nz + 2, step, 0)

    def drain(zz, _):
        @pl.when((zz <= z) & (z < nz - 1))
        def _():
            for i in range(PIECES):
                along_z(here(zz, x), zz, True, i).wait_send()

        @pl.when((zz >= z) & (z > 0))
        def _():
            for i in range(PIECES):
                along_z(here(zz, x), zz, False, i).wait_send()

        for way in (0, 1):
            along_x(here(zz, x), zz, x, way).wait_send()
            half_on(zz, left if way == 0 else right, way).wait_send()
        for xx in range(nx):
            across(here(zz, xx), zz, xx).wait_send()
            at = zz * nx + xx
            other = out.at[slot(zz, xx, 1 - core)]
            remote(other, other, ps.at[at], pr.at[at], {CORE: 1 - core}).wait_recv()
        return 0

    lax.fori_loop(0, nz, drain, 0)
    own.wait()


def gathered(blk, nz, nx):
    shape = (nz * nx * 2, *blk.shape)
    return pl.pallas_call(
        functools.partial(gather_kernel, nz, nx),
        out_shape=jax.ShapeDtypeStruct(shape, blk.dtype),
        in_specs=[VMEM],
        out_specs=VMEM,
        scratch_shapes=[
            DMA((2, nz, PIECES)),
            DMA((nz, PIECES)),
            DMA((2, nz)),
            DMA((2, nz)),
            DMA((2, nz)),
            DMA((2, nz)),
            DMA((nz * nx,)),
            DMA((nz * nx,)),
            DMA,
        ],
        compiler_params=pltpu.CompilerParams(
            collective_id=0, has_side_effects=True, vmem_limit_bytes=8 * 1024 * 1024
        ),
        name="gather",
    )(blk)


def attend_kernel(
    group,
    head,
    half,
    scale,
    stash,
    own_ids,
    queries,
    grads,
    blocks,
    dq,
    dkv,
    q_full,
    qs,
    gs,
    tops,
    totals,
    deltas,
    dq_sum,
    scores,
    dprobs,
    where_is,
    id_rows,
    ids,
    sems,
):
    total = 2 * blocks.shape[0]
    per = 256 // half
    tiles = total // per
    rows = group * half
    fetch = pltpu.make_async_copy(queries.at[0, stash[0]], q_full, sems.at[0])
    fetch.start()

    numbers = blocks[:, 4 * half :, :].astype(jnp.float32)
    id_rows[...] = jnp.max(numbers, axis=1).astype(jnp.int32)
    listing = pltpu.make_async_copy(id_rows, ids, sems.at[1])
    listing.start()
    low_first = (own_ids[0] < own_ids[1]).astype(jnp.int32)
    low = jnp.minimum(own_ids[0], own_ids[1])
    high = total - 1 - low
    halves = (low_first * half, (1 - low_first) * half)
    fetch.wait()
    for p in (0, 1):
        base = pl.multiple_of(halves[p], half)
        for h in range(group):
            cols = slice(h * head, (h + 1) * head)
            qs[p, h * half : (h + 1) * half, :] = q_full[pl.ds(base, half), cols]
            gs[p, h * half : (h + 1) * half, :] = grads[0, pl.ds(base, half), cols]
    tops[...] = jnp.full_like(tops, masked_score)
    totals[...] = jnp.zeros_like(totals)
    deltas[...] = jnp.zeros_like(deltas)
    dq_sum[...] = jnp.zeros_like(dq_sum)

    listing.wait()

    def place(i, _):
        where_is[ids[i, 0]] = 2 * i
        where_is[ids[i, head // 2]] = 2 * i + 1
        return 0

    lax.fori_loop(0, total // 2, place, 0)
    high_tiles = high // per + 1
    exp_scale = scale * math.log2(math.e)
    gap = lax.broadcasted_iota(jnp.int32, (256, rows), 0) - (
        lax.broadcasted_iota(jnp.int32, (256, rows), 1) % half
    )

    def unit(u):
        p = (u >= high_tiles).astype(jnp.int32)
        return p, u - p * high_tiles

    def tile_of(tile, first):
        pieces = []
        for i in range(per):
            at = where_is[tile * per + i]
            start = pl.multiple_of(first + (at % 2) * half, half)
            pieces.append(blocks[at // 2, pl.ds(start, half), :])
        return jnp.concatenate(pieces, axis=0)

    def cross(a, b, dims):
        return lax.dot_general(a, b, (dims, ((), ())), preferred_element_type=jnp.float32)

    def forward(u):
        p, tile = unit(u)
        mine = jnp.where(p == 0, high, low)
        t = cross(tile_of(tile, 0), qs[p], ((1,), (1,))) * exp_scale
        t = jnp.where(gap <= mine * half - tile * 256, t, masked_score)
        dprob = cross(tile_of(tile, 2 * half), gs[p], ((1,), (1,)))
        scores[u] = t
        dprobs[u] = dprob
        old = tops[p]
        new = jnp.maximum(old, jnp.max(t, axis=0, keepdims=True))
        fading = jnp.exp2(old - new)
        e = jnp.exp2(t - new)
        tops[p] = new
        totals[p] = totals[p] * fading + jnp.sum(e, axis=0, keepdims=True)
        deltas[p] = deltas[p] * fading + jnp.sum(e * dprob, axis=0, keepdims=True)

    units = tiles + 1
    together = 11 if units % 11 == 0 else 1

    def forward_step(i, _):
        for k in range(together):
            forward(i * together + k)
        return 0

    lax.fori_loop(0, units // together, forward_step, 0)
    deltas[...] = deltas[...] / totals[...]
    tops[...] = tops[...] + jnp.log2(totals[...])

    def backward(u):
        p, tile = unit(u)
        weights = jnp.exp2(scores[u] - tops[p])
        probs = weights.astype(jnp.bfloat16)
        dscore = (weights * (dprobs[u] - deltas[p]) * scale).astype(jnp.bfloat16)
        dk = cross(dscore, qs[p], ((1,), (0,)))
        dv = cross(probs, gs[p], ((1,), (0,)))
        dq_sum[p] += cross(tile_of(tile, 0), dscore, ((0,), (0,)))
        for i in range(per):
            at = where_is[tile * per + i]
            here = slice(i * half, (i + 1) * half)
            for part, first in ((dk, 0), (dv, 2 * half)):
                spot = (at // 2, pl.ds(pl.multiple_of(first + (at % 2) * half, half), half))
                before = jnp.where(p == 1, dkv[spot].astype(jnp.float32), 0.0)
                dkv[spot] = (before + part[here]).astype(jnp.bfloat16)

    def backward_step(i, _):
        for k in range(together):
            backward(i * together + k)
        return 0

    lax.fori_loop(0, units // together, backward_step, 0)

    def clear(s, _):
        at = where_is[s]
        for first in (0, 2 * half):
            spot = (at // 2, pl.ds(pl.multiple_of(first + (at % 2) * half, half), half))
            dkv[spot] = jnp.zeros((half, head), jnp.bfloat16)
        return 0

    lax.fori_loop(high_tiles * per, total, clear, 0)
    for p in (0, 1):
        base = pl.multiple_of(halves[p], half)
        turned = dq_sum[p].T.astype(jnp.bfloat16)
        for h in range(group):
            dq[pl.ds(base, half), h * head : (h + 1) * head] = turned[h * half : (h + 1) * half]


def attended(stash, own_ids, queries, grads, blocks, head):
    tokens, width = queries.shape[2:]
    group, half = width // head, tokens // 2
    rows = group * half
    total = 2 * blocks.shape[0]
    units = total * half // 256 + 1
    return pl.pallas_call(
        functools.partial(attend_kernel, group, head, half, 1.0 / math.sqrt(head)),
        out_shape=(
            jax.ShapeDtypeStruct((tokens, width), jnp.bfloat16),
            jax.ShapeDtypeStruct((blocks.shape[0], 2 * tokens, head), jnp.bfloat16),
        ),
        in_specs=[SMEM, SMEM, ANY, VMEM, VMEM],
        out_specs=(VMEM, VMEM),
        scratch_shapes=[
            pltpu.VMEM((tokens, width), jnp.bfloat16),
            pltpu.VMEM((2, rows, head), jnp.bfloat16),
            pltpu.VMEM((2, rows, head), jnp.bfloat16),
            pltpu.VMEM((2, 1, rows), jnp.float32),
            pltpu.VMEM((2, 1, rows), jnp.float32),
            pltpu.VMEM((2, 1, rows), jnp.float32),
            pltpu.VMEM((2, head, rows), jnp.float32),
            pltpu.VMEM((units, 256, rows), jnp.float32),
            pltpu.VMEM((units, 256, rows), jnp.float32),
            pltpu.SMEM((total,), jnp.int32),
            pltpu.VMEM((total // 2, head), jnp.int32),
            pltpu.SMEM((total // 2, head), jnp.int32),
            DMA((2,)),
        ],
        compiler_params=pltpu.CompilerParams(vmem_limit_bytes=32 * 1024 * 1024),
        name="attend",
    )(stash, own_ids, queries, grads, blocks)


def scatter_kernel(
    nz, nx, ns, dq, dkv, out, rx, held, hbuf, xbuf, zbuf, last, ps, pr, hs, hr, xs, xr, zs, zr, ms, mr
):
    z, x, core, right, left, far = neighbours(nz, nx)
    section = lax.axis_index(SECTION)
    ahead = lax.rem(section + ns - 1, ns)
    behind = lax.rem(section + 1, ns)
    tokens, width = dq.shape
    head = dkv.shape[2]
    ways = (right, left)

    barrier = pltpu.get_barrier_semaphore()
    pl.semaphore_signal(barrier, inc=1, device_id={SECTION: behind}, device_id_type=MESH)
    greet(nz, z, core, right, left, more=1)

    def pair(zz, xx):
        at = zz * nx + xx
        src = dkv.at[at * 2 + 1 - core]
        return remote(src, rx.at[at], ps.at[at], pr.at[at], {CORE: 1 - core})

    def nth(k):
        return jnp.where(k % 2 == 0, k // 2, nz - 1 - k // 2)

    main = remote(dq, out.at[:, pl.ds(0, width)], ms.at[0], mr.at[0], {SECTION: ahead})

    main.start()

    def launch(k, _):
        for xx in range(nx):
            pair(nth(k), xx).start()
        return 0

    lax.fori_loop(0, nz, launch, 0)

    def mine(zz, xx):
        at = zz * nx + xx
        return dkv[at * 2 + core].astype(jnp.float32) + rx[at].astype(jnp.float32)

    def half_on(zz, way):
        piece = held.at[zz, 0, pl.ds(way * tokens, tokens)]
        return remote(piece, hbuf.at[way, zz], hs.at[way, zz], hr.at[way, zz], {X: ways[way]})

    def along_x(zz, way):
        return remote(
            held.at[zz, 1 + way], xbuf.at[way, zz], xs.at[way, zz], xr.at[way, zz], {X: ways[way]}
        )

    def first(zz):
        for xx in range(nx):
            pair(zz, xx).wait_recv()
        held[zz, 0] = mine(zz, far).astype(jnp.bfloat16)
        half_on(zz, 0).start()
        half_on(zz, 1).start()

    def second(zz):
        for way in (0, 1):
            half_on(zz, way).wait_recv()
            own = mine(zz, ways[way])
            more = hbuf[way, zz].astype(jnp.float32)
            keep = (1 - way) * tokens
            joined = own[way * tokens : (way + 1) * tokens] + more
            held[zz, 1 + way, way * tokens : (way + 1) * tokens] = joined.astype(jnp.bfloat16)
            held[zz, 1 + way, keep : keep + tokens] = own[keep : keep + tokens].astype(jnp.bfloat16)
            along_x(zz, way).start()

    def third(zz):
        along_x(zz, 0).wait_recv()
        along_x(zz, 1).wait_recv()
        done = mine(zz, x) + xbuf[0, zz].astype(jnp.float32) + xbuf[1, zz].astype(jnp.float32)
        held[zz, 3] = done.astype(jnp.bfloat16)

    pieces = (pl.ds(0, tokens), pl.ds(tokens, tokens))

    def along_z(zz, down, piece):
        to = z - 1 if down else z + 1
        way = 0 if down else 1
        return remote(
            held.at[zz, 3, pieces[piece]],
            zbuf.at[way, zz, pieces[piece]],
            zs.at[way, zz, piece],
            zr.at[way, zz, piece],
            {Z: to},
        )

    def chain(zz, down, source):
        way = 0 if down else 1
        for piece in (0, 1):

            @pl.when(source)
            def _():
                along_z(zz, down, piece).wait_recv()
                joined = held[zz, 3, pieces[piece]].astype(jnp.float32) + zbuf[
                    way, zz, pieces[piece]
                ].astype(jnp.float32)
                held[zz, 3, pieces[piece]] = joined.astype(jnp.bfloat16)

            along_z(zz, down, piece).start()

    def up_chain(t):
        i = t - z

        @pl.when((i >= 0) & (i < nz - 1 - z))
        def _():
            chain(nz - 1 - i, False, z > 0)

    def down_chain(t):
        i = t - (nz - 1 - z)

        @pl.when((i >= 0) & (i < z))
        def _():
            chain(i, True, z < nz - 1)

    def step(k, _):
        @pl.when(k < nz)
        def _():
            first(nth(k))

        @pl.when((k >= 1) & (k <= nz))
        def _():
            second(nth(k - 1))

        @pl.when((k >= 2) & (k <= nz + 1))
        def _():
            third(nth(k - 2))

        @pl.when((k >= 3) & ((k % 2 == 1) | (k > nz + 1)))
        def _():
            t = jnp.where(k > nz + 1, k - (nz + 2) + nz // 2, (k - 3) // 2)
            up_chain(t)
            down_chain(t)

        return 0

    lax.fori_loop(0, nz + 2 + nz - 1 - nz // 2, step, 0)

    def tail(piece):
        return remote(
            held.at[z, 3, pieces[piece]],
            out.at[:, pl.ds(width + piece * head, head)],
            ms.at[1 + piece],
            mr.at[1 + piece],
            {SECTION: ahead},
        )

    for piece in (0, 1):
        last[pieces[piece]] = held[z, 3, pieces[piece]].astype(jnp.float32)

        @pl.when(z < nz - 1)
        def _():
            along_z(z, True, piece).wait_recv()
            last[pieces[piece]] += zbuf[0, z, pieces[piece]].astype(jnp.float32)

        @pl.when(z > 0)
        def _():
            along_z(z, False, piece).wait_recv()
            last[pieces[piece]] += zbuf[1, z, pieces[piece]].astype(jnp.float32)

        held[z, 3, pieces[piece]] = last[pieces[piece]].astype(jnp.bfloat16)
        tail(piece).start()

    def drain(zz, _):
        for xx in range(nx):
            pair(zz, xx).wait_send()
        for way in (0, 1):
            half_on(zz, way).wait_send()
            along_x(zz, way).wait_send()
        for piece in (0, 1):

            @pl.when(zz < z)
            def _():
                along_z(zz, True, piece).wait_send()

            @pl.when(zz > z)
            def _():
                along_z(zz, False, piece).wait_send()

        return 0

    lax.fori_loop(0, nz, drain, 0)
    main.wait()
    for piece in (0, 1):
        tail(piece).wait()


def scattered(dq, dkv, nz, nx, ns):
    tokens, width = dq.shape
    rows, head = dkv.shape[1:]
    half = jnp.bfloat16
    return pl.pallas_call(
        functools.partial(scatter_kernel, nz, nx, ns),
        out_shape=jax.ShapeDtypeStruct((tokens, width + 2 * head), half),
        in_specs=[VMEM, VMEM],
        out_specs=VMEM,
        scratch_shapes=[
            pltpu.VMEM((nz * nx, rows, head), half),
            pltpu.VMEM((nz, 4, rows, head), half),
            pltpu.VMEM((2, nz, rows // 2, head), half),
            pltpu.VMEM((2, nz, rows, head), half),
            pltpu.VMEM((2, nz, rows, head), half),
            pltpu.VMEM((rows, head), jnp.float32),
            DMA((nz * nx,)),
            DMA((nz * nx,)),
            DMA((2, nz)),
            DMA((2, nz)),
            DMA((2, nz)),
            DMA((2, nz)),
            DMA((2, nz, 2)),
            DMA((2, nz, 2)),
            DMA((3,)),
            DMA((3,)),
        ],
        compiler_params=pltpu.CompilerParams(
            collective_id=1, has_side_effects=True, vmem_limit_bytes=16 * 1024 * 1024
        ),
        name="scatter",
    )(dq, dkv)


def pack_kernel(stash, own_ids, keys, values, blk, sems):
    rows = keys.shape[2]
    parts = []
    for i, source in enumerate((keys, values)):
        part = pltpu.make_async_copy(
            source.at[0, stash[0]], blk.at[pl.ds(i * rows, rows)], sems.at[i]
        )
        part.start()
        parts.append(part)
    lane = lax.broadcasted_iota(jnp.int32, (ID_ROWS, blk.shape[1]), 1)
    numbers = jnp.where(lane < blk.shape[1] // 2, own_ids[0], own_ids[1])
    blk[2 * rows :, :] = numbers.astype(jnp.float32).astype(jnp.bfloat16)
    for part in parts:
        part.wait()


def packed(stash, own_ids, keys, values):
    rows, head = keys.shape[2:]
    return pl.pallas_call(
        pack_kernel,
        out_shape=jax.ShapeDtypeStruct((2 * rows + ID_ROWS, head), keys.dtype),
        in_specs=[SMEM, SMEM, IN_HBM, IN_HBM],
        out_specs=VMEM,
        scratch_shapes=[DMA((2,))],
        compiler_params=pltpu.CompilerParams(vmem_limit_bytes=VMEM_LIMIT),
        name="pack",
    )(stash, own_ids, keys, values)


def per_device(sizes, queries, keys, values, out_grad, stretch_ids, stash_slot):
    ns, nz, nx = sizes
    head = keys.shape[3]
    blk = packed(stash_slot, stretch_ids, keys, values)
    blocks = gathered(blk, nz, nx)
    dq, dkv = attended(stash_slot, stretch_ids, queries, out_grad, blocks, head)
    return scattered(dq, dkv, nz, nx, ns)[None]


def solution(mesh):
    ns = mesh.shape["section"]
    nz, nx = 8, 4
    split = Mesh(mesh.devices.reshape(ns, nz, nx, 2), (SECTION, Z, X, CORE))
    return jax.shard_map(
        functools.partial(per_device, (ns, nz, nx)),
        mesh=split,
        in_specs=(
            P(SECTION, None, CTX, None),
            P(SECTION, None, CTX, None),
            P(SECTION, None, CTX, None),
            P(SECTION, CTX, None),
            P(CTX),
            P(SECTION),
        ),
        out_specs=P(SECTION, CTX, None),
        check_vma=False,
    )
```

```python
import functools
import math

import jax
import jax.numpy as jnp
from jax import lax
from jax.experimental import pallas as pl
from jax.experimental.pallas import tpu as pltpu
from jax.sharding import Mesh
from jax.sharding import PartitionSpec as P

Z, X, CORE, SECTION = "ctx_0", "ctx_1", "ctx_2", "section"
CTX = (Z, X, CORE)
MESH = pl.DeviceIdType.MESH
VMEM = pl.BlockSpec(memory_space=pltpu.VMEM)
SMEM = pl.BlockSpec(memory_space=pltpu.SMEM)
ANY = pl.BlockSpec(memory_space=pl.ANY)
IN_HBM = pl.BlockSpec(memory_space=pltpu.HBM)
DMA = pltpu.SemaphoreType.DMA
VMEM_LIMIT = 60 * 1024 * 1024

ID_ROWS = 16
PIECES = 2
SUM_PIECES = 4
masked_score = -1e30


def neighbours(nz, nx):
    z, x, core = lax.axis_index(Z), lax.axis_index(X), lax.axis_index(CORE)
    right = lax.rem(x + 1, nx)
    left = lax.rem(x + nx - 1, nx)
    far = lax.rem(x + nx // 2, nx)
    return z, x, core, right, left, far


def greet(nz, z, core, right, left, more=0):
    barrier = pltpu.get_barrier_semaphore()

    def signal(**where):
        pl.semaphore_signal(barrier, inc=1, device_id=dict(where), device_id_type=MESH)

    signal(**{X: right})
    signal(**{X: left})
    signal(**{CORE: 1 - core})

    @pl.when(z > 0)
    def _():
        signal(**{Z: z - 1})

    @pl.when(z < nz - 1)
    def _():
        signal(**{Z: z + 1})

    inside = (z > 0).astype(jnp.int32) + (z < nz - 1).astype(jnp.int32)
    pl.semaphore_wait(barrier, 3 + more + inside)


def remote(src, dst, send, recv, where):
    return pltpu.make_async_remote_copy(
        src_ref=src, dst_ref=dst, send_sem=send, recv_sem=recv, device_id=where, device_id_type=MESH
    )


def gather_kernel(nz, nx, blk, out, zs, zr, xs, xr, hs, hr, ps, pr, own_sem):
    z, x, core, right, left, far = neighbours(nz, nx)
    rows = blk.shape[0]
    cut = rows // 2 // 16 * 16
    halves = (pl.ds(0, cut), pl.ds(cut, rows - cut))
    size = rows // PIECES // 16 * 16
    pieces = [pl.ds(i * size, size if i < PIECES - 1 else rows - i * size) for i in range(PIECES)]

    def slot(zz, xx, cc):
        return (zz * nx + xx) * 2 + cc

    own = pltpu.make_async_copy(blk, out.at[slot(z, x, core)], own_sem)
    own.start()
    greet(nz, z, core, right, left)

    def along_z(src, zz, up, i):
        to = z + 1 if up else z - 1
        return remote(
            src.at[pieces[i]],
            out.at[slot(zz, x, core), pieces[i]],
            zs.at[0 if up else 1, zz, i],
            zr.at[zz, i],
            {Z: to},
        )

    def along_x(src, zz, xx, way):
        to = right if way == 0 else left
        return remote(src, out.at[slot(zz, xx, core)], xs.at[way, zz], xr.at[way, zz], {X: to})

    def half_on(zz, xx, way):
        to = right if way == 0 else left
        piece = out.at[slot(zz, xx, core), halves[way]]
        return remote(piece, piece, hs.at[way, zz], hr.at[way, zz], {X: to})

    def across(src, zz, xx):
        at = zz * nx + xx
        return remote(src, out.at[slot(zz, xx, core)], ps.at[at], pr.at[at], {CORE: 1 - core})

    def here(zz, xx):
        return out.at[slot(zz, xx, core)]

    def spread(src, zz):
        along_x(src, zz, x, 0).start()
        along_x(src, zz, x, 1).start()
        across(src, zz, x).start()

    @pl.when(z < nz - 1)
    def _():
        for i in range(PIECES):
            along_z(blk, z, True, i).start()

    @pl.when(z > 0)
    def _():
        for i in range(PIECES):
            along_z(blk, z, False, i).start()

    spread(blk, z)

    def z_stage(s):
        @pl.when(z - s >= 0)
        def _():
            zz = z - s
            for i in range(PIECES):
                along_z(here(zz, x), zz, True, i).wait_recv()

                @pl.when(z < nz - 1)
                def _():
                    along_z(here(zz, x), zz, True, i).start()

            spread(here(zz, x), zz)

        @pl.when(z + s <= nz - 1)
        def _():
            zz = z + s
            for i in range(PIECES):
                along_z(here(zz, x), zz, False, i).wait_recv()

                @pl.when(z > 0)
                def _():
                    along_z(here(zz, x), zz, False, i).start()

            spread(here(zz, x), zz)

    def x_one(zz):
        along_x(here(zz, left), zz, left, 0).wait_recv()
        half_on(zz, left, 0).start()
        across(here(zz, left), zz, left).start()
        along_x(here(zz, right), zz, right, 1).wait_recv()
        half_on(zz, right, 1).start()
        across(here(zz, right), zz, right).start()

    def h_one(zz):
        half_on(zz, far, 0).wait_recv()
        half_on(zz, far, 1).wait_recv()
        across(here(zz, far), zz, far).start()

    def both_ways(one, t):
        @pl.when(z - t >= 0)
        def _():
            one(z - t)

        @pl.when((t > 0) & (z + t <= nz - 1))
        def _():
            one(z + t)

    def step(s, _):
        @pl.when(s < nz)
        def _():
            z_stage(s)

        @pl.when(s <= nz)
        def _():
            both_ways(x_one, s - 1)

        @pl.when(s >= 2)
        def _():
            both_ways(h_one, s - 2)

        return 0

    lax.fori_loop(1, nz + 2, step, 0)

    def drain(zz, _):
        @pl.when((zz <= z) & (z < nz - 1))
        def _():
            for i in range(PIECES):
                along_z(here(zz, x), zz, True, i).wait_send()

        @pl.when((zz >= z) & (z > 0))
        def _():
            for i in range(PIECES):
                along_z(here(zz, x), zz, False, i).wait_send()

        for way in (0, 1):
            along_x(here(zz, x), zz, x, way).wait_send()
            half_on(zz, left if way == 0 else right, way).wait_send()
        for xx in range(nx):
            across(here(zz, xx), zz, xx).wait_send()
            at = zz * nx + xx
            other = out.at[slot(zz, xx, 1 - core)]
            remote(other, other, ps.at[at], pr.at[at], {CORE: 1 - core}).wait_recv()
        return 0

    lax.fori_loop(0, nz, drain, 0)
    own.wait()


def gathered(blk, nz, nx):
    shape = (nz * nx * 2, *blk.shape)
    return pl.pallas_call(
        functools.partial(gather_kernel, nz, nx),
        out_shape=jax.ShapeDtypeStruct(shape, blk.dtype),
        in_specs=[VMEM],
        out_specs=VMEM,
        scratch_shapes=[
            DMA((2, nz, PIECES)),
            DMA((nz, PIECES)),
            DMA((2, nz)),
            DMA((2, nz)),
            DMA((2, nz)),
            DMA((2, nz)),
            DMA((nz * nx,)),
            DMA((nz * nx,)),
            DMA,
        ],
        compiler_params=pltpu.CompilerParams(
            collective_id=0, has_side_effects=True, vmem_limit_bytes=8 * 1024 * 1024
        ),
        name="gather",
    )(blk)


def attend_kernel(
    group,
    head,
    half,
    scale,
    stash,
    own_ids,
    queries,
    grads,
    blocks,
    dq,
    dkv,
    q_full,
    qs,
    gs,
    qt,
    gt,
    tops,
    totals,
    deltas,
    dq_sum,
    scores,
    dprobs,
    where_is,
    id_rows,
    ids,
    sems,
):
    total = 2 * blocks.shape[0]
    per = 256 // half
    tiles = total // per
    rows = group * half
    fetch = pltpu.make_async_copy(queries.at[0, stash[0]], q_full, sems.at[0])
    fetch.start()

    numbers = blocks[:, 4 * half :, :].astype(jnp.float32)
    id_rows[...] = jnp.max(numbers, axis=1).astype(jnp.int32)
    listing = pltpu.make_async_copy(id_rows, ids, sems.at[1])
    listing.start()
    low_first = (own_ids[0] < own_ids[1]).astype(jnp.int32)
    low = jnp.minimum(own_ids[0], own_ids[1])
    high = total - 1 - low
    halves = (low_first * half, (1 - low_first) * half)
    fetch.wait()
    for p in (0, 1):
        base = pl.multiple_of(halves[p], half)
        for h in range(group):
            cols = slice(h * head, (h + 1) * head)
            qs[p, h * half : (h + 1) * half, :] = q_full[pl.ds(base, half), cols]
            gs[p, h * half : (h + 1) * half, :] = grads[0, pl.ds(base, half), cols]
    for p in (0, 1):
        qt[p] = qs[p].T
        gt[p] = gs[p].T
    tops[...] = jnp.full_like(tops, masked_score)
    totals[...] = jnp.zeros_like(totals)
    deltas[...] = jnp.zeros_like(deltas)
    dq_sum[...] = jnp.zeros_like(dq_sum)

    listing.wait()

    def place(i, _):
        where_is[ids[i, 0]] = 2 * i
        where_is[ids[i, head // 2]] = 2 * i + 1
        return 0

    lax.fori_loop(0, total // 2, place, 0)
    high_tiles = high // per + 1
    exp_scale = scale * math.log2(math.e)
    gap = lax.broadcasted_iota(jnp.int32, (256, rows), 0) - (
        lax.broadcasted_iota(jnp.int32, (256, rows), 1) % half
    )

    def unit(u):
        p = (u >= high_tiles).astype(jnp.int32)
        return p, u - p * high_tiles

    def tile_of(tile, first):
        pieces = []
        for i in range(per):
            at = where_is[tile * per + i]
            start = pl.multiple_of(first + (at % 2) * half, half)
            pieces.append(blocks[at // 2, pl.ds(start, half), :])
        return jnp.concatenate(pieces, axis=0)

    def cross(a, b, dims):
        return lax.dot_general(a, b, (dims, ((), ())), preferred_element_type=jnp.float32)

    def forward(u):
        p, tile = unit(u)
        mine = jnp.where(p == 0, high, low)
        t = cross(tile_of(tile, 0), qt[p], ((1,), (0,))) * exp_scale
        t = jnp.where(gap <= mine * half - tile * 256, t, masked_score)
        dprob = cross(tile_of(tile, 2 * half), gt[p], ((1,), (0,)))
        scores[u] = t
        dprobs[u] = dprob
        old = tops[p]
        new = jnp.maximum(old, jnp.max(t, axis=0, keepdims=True))
        fading = jnp.exp2(old - new)
        e = jnp.exp2(t - new)
        tops[p] = new
        totals[p] = totals[p] * fading + jnp.sum(e, axis=0, keepdims=True)
        deltas[p] = deltas[p] * fading + jnp.sum(e * dprob, axis=0, keepdims=True)

    units = tiles + 1
    together = 11 if units % 11 == 0 else 1

    def forward_step(i, _):
        for k in range(together):
            forward(i * together + k)
        return 0

    lax.fori_loop(0, units // together, forward_step, 0)
    deltas[...] = deltas[...] / totals[...]
    tops[...] = tops[...] + jnp.log2(totals[...])

    def backward(u):
        p, tile = unit(u)
        weights = jnp.exp2(scores[u] - tops[p])
        probs = weights.astype(jnp.bfloat16)
        dscore = (weights * (dprobs[u] - deltas[p]) * scale).astype(jnp.bfloat16)
        dk = cross(dscore, qs[p], ((1,), (0,)))
        dv = cross(probs, gs[p], ((1,), (0,)))
        dq_sum[p] += cross(tile_of(tile, 0), dscore, ((0,), (0,)))
        for i in range(per):
            at = where_is[tile * per + i]
            here = slice(i * half, (i + 1) * half)
            for part, first in ((dk, 0), (dv, 2 * half)):
                spot = (at // 2, pl.ds(pl.multiple_of(first + (at % 2) * half, half), half))
                before = jnp.where(p == 1, dkv[spot].astype(jnp.float32), 0.0)
                dkv[spot] = (before + part[here]).astype(jnp.bfloat16)

    def backward_step(i, _):
        for k in range(together):
            backward(i * together + k)
        return 0

    lax.fori_loop(0, units // together, backward_step, 0)

    def clear(s, _):
        at = where_is[s]
        for first in (0, 2 * half):
            spot = (at // 2, pl.ds(pl.multiple_of(first + (at % 2) * half, half), half))
            dkv[spot] = jnp.zeros((half, head), jnp.bfloat16)
        return 0

    lax.fori_loop(high_tiles * per, total, clear, 0)
    for p in (0, 1):
        base = pl.multiple_of(halves[p], half)
        turned = dq_sum[p].T.astype(jnp.bfloat16)
        for h in range(group):
            dq[pl.ds(base, half), h * head : (h + 1) * head] = turned[h * half : (h + 1) * half]


def attended(stash, own_ids, queries, grads, blocks, head):
    tokens, width = queries.shape[2:]
    group, half = width // head, tokens // 2
    rows = group * half
    total = 2 * blocks.shape[0]
    units = total * half // 256 + 1
    return pl.pallas_call(
        functools.partial(attend_kernel, group, head, half, 1.0 / math.sqrt(head)),
        out_shape=(
            jax.ShapeDtypeStruct((tokens, width), jnp.bfloat16),
            jax.ShapeDtypeStruct((blocks.shape[0], 2 * tokens, head), jnp.bfloat16),
        ),
        in_specs=[SMEM, SMEM, ANY, VMEM, VMEM],
        out_specs=(VMEM, VMEM),
        scratch_shapes=[
            pltpu.VMEM((tokens, width), jnp.bfloat16),
            pltpu.VMEM((2, rows, head), jnp.bfloat16),
            pltpu.VMEM((2, rows, head), jnp.bfloat16),
            pltpu.VMEM((2, head, rows), jnp.bfloat16),
            pltpu.VMEM((2, head, rows), jnp.bfloat16),
            pltpu.VMEM((2, 1, rows), jnp.float32),
            pltpu.VMEM((2, 1, rows), jnp.float32),
            pltpu.VMEM((2, 1, rows), jnp.float32),
            pltpu.VMEM((2, head, rows), jnp.float32),
            pltpu.VMEM((units, 256, rows), jnp.float32),
            pltpu.VMEM((units, 256, rows), jnp.float32),
            pltpu.SMEM((total,), jnp.int32),
            pltpu.VMEM((total // 2, head), jnp.int32),
            pltpu.SMEM((total // 2, head), jnp.int32),
            DMA((2,)),
        ],
        compiler_params=pltpu.CompilerParams(vmem_limit_bytes=32 * 1024 * 1024),
        name="attend",
    )(stash, own_ids, queries, grads, blocks)


def scatter_kernel(
    nz, nx, ns, dq, dkv, out, rx, held, hbuf, xbuf, zbuf, last, ps, pr, hs, hr, xs, xr, zs, zr, ms, mr
):
    z, x, core, right, left, far = neighbours(nz, nx)
    section = lax.axis_index(SECTION)
    ahead = lax.rem(section + ns - 1, ns)
    behind = lax.rem(section + 1, ns)
    tokens, width = dq.shape
    head = dkv.shape[2]
    ways = (right, left)

    barrier = pltpu.get_barrier_semaphore()
    pl.semaphore_signal(barrier, inc=1, device_id={SECTION: behind}, device_id_type=MESH)
    greet(nz, z, core, right, left, more=1)

    def pair(zz, xx):
        at = zz * nx + xx
        src = dkv.at[at * 2 + 1 - core]
        return remote(src, rx.at[at], ps.at[at], pr.at[at], {CORE: 1 - core})

    def nth(k):
        return jnp.where(k % 2 == 0, k // 2, nz - 1 - k // 2)

    main = remote(dq, out.at[:, pl.ds(0, width)], ms.at[0], mr.at[0], {SECTION: ahead})

    main.start()

    def launch(k, _):
        for xx in range(nx):
            pair(nth(k), xx).start()
        return 0

    lax.fori_loop(0, nz, launch, 0)

    def mine(zz, xx):
        at = zz * nx + xx
        return dkv[at * 2 + core].astype(jnp.float32) + rx[at].astype(jnp.float32)

    def half_on(zz, way):
        piece = held.at[zz, 0, pl.ds(way * tokens, tokens)]
        return remote(piece, hbuf.at[way, zz], hs.at[way, zz], hr.at[way, zz], {X: ways[way]})

    def along_x(zz, way):
        return remote(
            held.at[zz, 1 + way], xbuf.at[way, zz], xs.at[way, zz], xr.at[way, zz], {X: ways[way]}
        )

    def first(zz):
        for xx in range(nx):
            pair(zz, xx).wait_recv()
        held[zz, 0] = mine(zz, far).astype(jnp.bfloat16)
        half_on(zz, 0).start()
        half_on(zz, 1).start()

    def second(zz):
        for way in (0, 1):
            half_on(zz, way).wait_recv()
            own = mine(zz, ways[way])
            more = hbuf[way, zz].astype(jnp.float32)
            keep = (1 - way) * tokens
            joined = own[way * tokens : (way + 1) * tokens] + more
            held[zz, 1 + way, way * tokens : (way + 1) * tokens] = joined.astype(jnp.bfloat16)
            held[zz, 1 + way, keep : keep + tokens] = own[keep : keep + tokens].astype(jnp.bfloat16)
            along_x(zz, way).start()

    def third(zz):
        along_x(zz, 0).wait_recv()
        along_x(zz, 1).wait_recv()
        done = mine(zz, x) + xbuf[0, zz].astype(jnp.float32) + xbuf[1, zz].astype(jnp.float32)
        held[zz, 3] = done.astype(jnp.bfloat16)

    pieces = (pl.ds(0, tokens), pl.ds(tokens, tokens))
    size = 2 * tokens // SUM_PIECES
    bits = [pl.ds(i * size, size) for i in range(SUM_PIECES)]

    def along_z(zz, down, piece):
        to = z - 1 if down else z + 1
        way = 0 if down else 1
        return remote(
            held.at[zz, 3, bits[piece]],
            zbuf.at[way, zz, bits[piece]],
            zs.at[way, zz, piece],
            zr.at[way, zz, piece],
            {Z: to},
        )

    def chain(zz, down, source):
        way = 0 if down else 1
        for piece in range(SUM_PIECES):

            @pl.when(source)
            def _():
                along_z(zz, down, piece).wait_recv()
                joined = held[zz, 3, bits[piece]].astype(jnp.float32) + zbuf[
                    way, zz, bits[piece]
                ].astype(jnp.float32)
                held[zz, 3, bits[piece]] = joined.astype(jnp.bfloat16)

            along_z(zz, down, piece).start()

    def up_chain(t):
        i = t - z

        @pl.when((i >= 0) & (i < nz - 1 - z))
        def _():
            chain(nz - 1 - i, False, z > 0)

    def down_chain(t):
        i = t - (nz - 1 - z)

        @pl.when((i >= 0) & (i < z))
        def _():
            chain(i, True, z < nz - 1)

    def step(k, _):
        @pl.when(k < nz)
        def _():
            first(nth(k))

        @pl.when((k >= 1) & (k <= nz))
        def _():
            second(nth(k - 1))

        @pl.when((k >= 2) & (k <= nz + 1))
        def _():
            third(nth(k - 2))

        @pl.when((k >= 3) & ((k % 2 == 1) | (k > nz + 1)))
        def _():
            t = jnp.where(k > nz + 1, k - (nz + 2) + nz // 2, (k - 3) // 2)
            up_chain(t)
            down_chain(t)

        return 0

    lax.fori_loop(0, nz + 2 + nz - 1 - nz // 2, step, 0)

    def tail(piece):
        return remote(
            held.at[z, 3, pieces[piece]],
            out.at[:, pl.ds(width + piece * head, head)],
            ms.at[1 + piece],
            mr.at[1 + piece],
            {SECTION: ahead},
        )

    share = SUM_PIECES // 2
    for piece in (0, 1):
        last[pieces[piece]] = held[z, 3, pieces[piece]].astype(jnp.float32)

        @pl.when(z < nz - 1)
        def _():
            for i in range(share * piece, share * piece + share):
                along_z(z, True, i).wait_recv()
            last[pieces[piece]] += zbuf[0, z, pieces[piece]].astype(jnp.float32)

        @pl.when(z > 0)
        def _():
            for i in range(share * piece, share * piece + share):
                along_z(z, False, i).wait_recv()
            last[pieces[piece]] += zbuf[1, z, pieces[piece]].astype(jnp.float32)

        held[z, 3, pieces[piece]] = last[pieces[piece]].astype(jnp.bfloat16)
        tail(piece).start()

    def drain(zz, _):
        for xx in range(nx):
            pair(zz, xx).wait_send()
        for way in (0, 1):
            half_on(zz, way).wait_send()
            along_x(zz, way).wait_send()
        for piece in range(SUM_PIECES):

            @pl.when(zz < z)
            def _():
                along_z(zz, True, piece).wait_send()

            @pl.when(zz > z)
            def _():
                along_z(zz, False, piece).wait_send()

        return 0

    lax.fori_loop(0, nz, drain, 0)
    main.wait()
    for piece in (0, 1):
        tail(piece).wait()


def scattered(dq, dkv, nz, nx, ns):
    tokens, width = dq.shape
    rows, head = dkv.shape[1:]
    half = jnp.bfloat16
    return pl.pallas_call(
        functools.partial(scatter_kernel, nz, nx, ns),
        out_shape=jax.ShapeDtypeStruct((tokens, width + 2 * head), half),
        in_specs=[VMEM, VMEM],
        out_specs=VMEM,
        scratch_shapes=[
            pltpu.VMEM((nz * nx, rows, head), half),
            pltpu.VMEM((nz, 4, rows, head), half),
            pltpu.VMEM((2, nz, rows // 2, head), half),
            pltpu.VMEM((2, nz, rows, head), half),
            pltpu.VMEM((2, nz, rows, head), half),
            pltpu.VMEM((rows, head), jnp.float32),
            DMA((nz * nx,)),
            DMA((nz * nx,)),
            DMA((2, nz)),
            DMA((2, nz)),
            DMA((2, nz)),
            DMA((2, nz)),
            DMA((2, nz, SUM_PIECES)),
            DMA((2, nz, SUM_PIECES)),
            DMA((3,)),
            DMA((3,)),
        ],
        compiler_params=pltpu.CompilerParams(
            collective_id=1, has_side_effects=True, vmem_limit_bytes=16 * 1024 * 1024
        ),
        name="scatter",
    )(dq, dkv)


def pack_kernel(stash, own_ids, keys, values, blk, sems):
    rows = keys.shape[2]
    parts = []
    for i, source in enumerate((keys, values)):
        part = pltpu.make_async_copy(
            source.at[0, stash[0]], blk.at[pl.ds(i * rows, rows)], sems.at[i]
        )
        part.start()
        parts.append(part)
    lane = lax.broadcasted_iota(jnp.int32, (ID_ROWS, blk.shape[1]), 1)
    numbers = jnp.where(lane < blk.shape[1] // 2, own_ids[0], own_ids[1])
    blk[2 * rows :, :] = numbers.astype(jnp.float32).astype(jnp.bfloat16)
    for part in parts:
        part.wait()


def packed(stash, own_ids, keys, values):
    rows, head = keys.shape[2:]
    return pl.pallas_call(
        pack_kernel,
        out_shape=jax.ShapeDtypeStruct((2 * rows + ID_ROWS, head), keys.dtype),
        in_specs=[SMEM, SMEM, IN_HBM, IN_HBM],
        out_specs=VMEM,
        scratch_shapes=[DMA((2,))],
        compiler_params=pltpu.CompilerParams(vmem_limit_bytes=VMEM_LIMIT),
        name="pack",
    )(stash, own_ids, keys, values)


def per_device(sizes, queries, keys, values, out_grad, stretch_ids, stash_slot):
    ns, nz, nx = sizes
    head = keys.shape[3]
    blk = packed(stash_slot, stretch_ids, keys, values)
    blocks = gathered(blk, nz, nx)
    dq, dkv = attended(stash_slot, stretch_ids, queries, out_grad, blocks, head)
    return scattered(dq, dkv, nz, nx, ns)[None]


def solution(mesh):
    ns = mesh.shape["section"]
    nz, nx = 8, 4
    split = Mesh(mesh.devices.reshape(ns, nz, nx, 2), (SECTION, Z, X, CORE))
    return jax.shard_map(
        functools.partial(per_device, (ns, nz, nx)),
        mesh=split,
        in_specs=(
            P(SECTION, None, CTX, None),
            P(SECTION, None, CTX, None),
            P(SECTION, None, CTX, None),
            P(SECTION, CTX, None),
            P(CTX),
            P(SECTION),
        ),
        out_specs=P(SECTION, CTX, None),
        check_vma=False,
    )
```
